32 devices in a mesh: chan: 8 (over y, x, core), tm: 4 (over z).
Axes of the slice: x: 2, y: 2, z: 4, core: 2. Of those that a mesh axis runs over, the one named last changes fastest.
Arguments:
- voltages: bfloat16 [2, 8, 2048, 512], P(None, None, 'chan', 'tm'), may hold values from -0.25 to 0.25
- assignment: int32 [1024, 1], replicated, may hold values from 0 to 7; in each aligned block of 1024 rows (0 to 1023, 1024 to 2047, ...) at most 192 rows name the same one
- slot_subarray_index: int32 [8], replicated, may hold values from 0 to 7, each once
Outputs:
- visibilities: float32 [8, 8, 2, 384, 384], P('tm', 'chan')
The draws below stay inside these ranges and needn't reach their ends.
Inputs may be any that keep to these rules, and one draw needn't show every extreme that they name: `assignment`: no subarray holds more than 192 antennas; one holds exactly 192. `slot_subarray_index`: each subarray appears once.
All inputs are finite; a program needn't handle non-finite values.
Results may differ from the reference program's by a relative error of at most 0.008.
Values may be sent and summed in bfloat16 or wider, within the bound.
No kernel may reach another device: no remote copies, remote signals or barrier semaphores. Data moves between devices by JAX's collectives and lax.ppermute only.
A program may use at most 64 MiB of HBM per device.

```python
import math
import jax
import jax.numpy as jnp
import numpy as np
from jax import lax

ANTENNA_TOTAL = 1024
SUBARRAY_TOTAL = 8
SAMPLES_LOCAL = 128
INPUTS = 2048
ANTENNA_LIMIT = 192
SLOT = 384
CHANS = 8
SAMPLES = 512
N_TM = 4


def steps_of(key, dims, shards, low, high):
    gain = 1.0
    for axis_at, shards_of in shards:
        steps = jax.random.uniform(jax.random.fold_in(jax.random.fold_in(key, 6), axis_at), (shards_of,), jnp.float32, low / len(shards), high / len(shards))
        gain = gain * jnp.repeat(jnp.exp(steps), dims[axis_at] // shards_of).reshape((-1,) + (1,) * (len(dims) - 1 - axis_at))
    return gain


def deal_out(stream_key, own, number, rows, count, top, bound, slope):
    order = jax.random.permutation(stream_key, count)
    crowded, ordinary = shares(count, rows * top, bound, slope, True), shares(count, rows * top, bound, slope, False)
    places = jnp.arange(count)

    def named(tallies, offset_by):
        used = int((tallies > 0).sum())
        fixed = max(1, used // 4)
        shifted = fixed + (places - fixed + offset_by * (used - fixed)) % max(1, count - fixed)
        return jnp.zeros((count,), jnp.int32).at[order[jnp.where(places < fixed, places, shifted)]].set(jnp.asarray(tallies, jnp.int32))

    tallies = jnp.where(number % 4 == 0, named(crowded, number // 4), named(ordinary, number - number // 4 - 1))
    mixed = jax.random.permutation(jax.random.fold_in(own, 3), count)
    giver, receiver = mixed[0:count // 2 * 2:2], mixed[1:count // 2 * 2:2]
    margin = jnp.minimum(tallies[giver] - 1, bound - tallies[receiver]) // 2
    margin = jnp.where((giver == order[0]) | (receiver == order[0]) | (tallies[receiver] == 0), 0, jnp.maximum(margin, 0))
    shifted = jax.random.randint(jax.random.fold_in(own, 4), (count // 2,), 0, 1 << 20) % (margin + 1)
    tallies = tallies.at[giver].add(-shifted).at[receiver].add(shifted)
    labels = jnp.searchsorted(jnp.cumsum(tallies), jnp.arange(rows * top), side="right").astype(jnp.int32)
    grid = labels.reshape(top, rows).T
    grid = grid[jax.random.permutation(jax.random.fold_in(own, 1), rows)]
    offset_by = jax.random.randint(jax.random.fold_in(own, 2), (rows, 1), 0, top)
    return jnp.take_along_axis(grid, (jnp.arange(top)[None, :] + offset_by) % top, axis=1)


def shares(number_of, total, limit, lean, full):
    weights = [(1 << 20) // math.isqrt(rank ** lean) + 1 for rank in range(1, number_of + 1)]
    largest = limit if full else min(limit, max(-(-total // number_of), total * weights[0] // sum(weights)))
    least = 1 if total - largest >= number_of - 1 else 0
    holding, spare = [largest] + [least] * (number_of - 1), total - largest - least * (number_of - 1)
    while spare > 0:
        free = [i for i in range(1, number_of) if holding[i] < largest] or [i for i in range(1, number_of) if holding[i] < limit]
        mass, remaining = sum([weights[i] for i in free]), spare
        for i in free:
            addition = min(limit - holding[i], max(1, remaining * weights[i] // mass), spare)
            holding[i] = holding[i] + addition
            spare = spare - addition
    return np.array(holding)


def scatter_about(rng, shape, scale, limit, pieces=(), kind=jnp.bfloat16):
    array = jax.random.normal(rng, shape, jnp.float32) * scale
    if len(pieces) > 0:
        array = steps_of(rng, shape, pieces, -0.22, 0.18) * array
    return jnp.clip(array, min=-limit, max=limit).astype(kind)


def setup_inputs(seed: int = 0) -> dict:
    seeds = jax.random.split(jax.random.key(seed), 4)
    voltages = scatter_about(seeds[0], (2, CHANS, INPUTS, SAMPLES), SAMPLES ** -0.5, 0.25, ((2, 8), (3, 4)))
    assignment_keys = jax.random.split(jax.random.fold_in(seeds[1], 1), ANTENNA_TOTAL // ANTENNA_TOTAL)
    assignment_turns = jax.random.permutation(jax.random.fold_in(seeds[1], 3), ANTENNA_TOTAL // ANTENNA_TOTAL)
    assignment = jax.vmap(lambda own, number: deal_out(jax.random.fold_in(seeds[1], 2), own, number, ANTENNA_TOTAL, SUBARRAY_TOTAL, 1, ANTENNA_LIMIT, 2))(assignment_keys, assignment_turns).reshape((ANTENNA_TOTAL, 1))
    slot_subarray_index = jax.random.permutation(seeds[2], SUBARRAY_TOTAL).astype(jnp.int32)
    return {"voltages": voltages, "assignment": assignment, "slot_subarray_index": slot_subarray_index}


def result_slot_lookup(assignment, slot_subarray_index):
    owner = jnp.repeat(assignment[:, 0], 2).astype(jnp.int32)
    onehot = (owner[:, None] == jnp.arange(SUBARRAY_TOTAL, dtype=jnp.int32)[None, :]).astype(jnp.int32)
    ranks = jnp.sum((jnp.cumsum(onehot, axis=0) - onehot) * onehot, axis=1).astype(jnp.int32)
    table = jnp.full((SUBARRAY_TOTAL, SLOT), INPUTS, jnp.int32)
    table = table.at[owner, ranks].set(jnp.arange(INPUTS, dtype=jnp.int32))
    return table[slot_subarray_index.astype(jnp.int32)].reshape(-1).astype(jnp.int32)


def compact(block, rows):
    parts, chans, inputs, samples = block.shape
    padded_voltages = jnp.concatenate([block, jnp.zeros((parts, chans, 1, samples), block.dtype)], axis=2)
    picked = jnp.take(padded_voltages, rows, axis=2)
    picked = picked.reshape(parts, chans, SUBARRAY_TOTAL, SLOT, samples)
    picked = jnp.transpose(picked, (2, 1, 0, 3, 4))
    return picked.reshape(SUBARRAY_TOTAL, chans, 2 * SLOT, samples)


def gram(stacked):
    stacked = stacked.astype(jnp.float32)
    full = jnp.einsum("...pt,...qt->...pq", stacked, stacked)
    half = stacked.shape[-2] // 2
    real = full[..., :half, :half] + full[..., half:, half:]
    imag = full[..., half:, :half] - full[..., :half, half:]
    return jnp.stack([real, imag], axis=-3)


def blocked_gram(stacked):
    total = None
    for block_index in range(N_TM):
        piece = stacked[..., block_index * SAMPLES_LOCAL:(block_index + 1) * SAMPLES_LOCAL]
        rounded = gram(piece).astype(jnp.bfloat16)
        rounded = lax.optimization_barrier(rounded).astype(jnp.float32)
        total = rounded if total is None else total + rounded
    return total


def reference(voltages, assignment, slot_subarray_index):
    rows = result_slot_lookup(assignment, slot_subarray_index)

    def one_channel(block):
        return blocked_gram(compact(block[:, None], rows))[:, 0]

    result = lax.map(one_channel, jnp.moveaxis(voltages, 1, 0))
    return jnp.transpose(result, (1, 0, 2, 3, 4))
```

```python
import functools

import jax
import jax.numpy as jnp
from jax import lax
from jax.experimental import pallas as pl
from jax.experimental.pallas import tpu as pltpu
from jax.sharding import PartitionSpec as P

SLOT = 384
LANES = 128

VMEM = pl.BlockSpec(memory_space=pltpu.VMEM)
SMEM = pl.BlockSpec(memory_space=pltpu.SMEM)
PARAMS = pltpu.CompilerParams(vmem_limit_bytes=20 * 1024 * 1024)


def partner(index, step, count):
    if count & (count - 1):
        return lax.rem(index + step, count) if not isinstance(index, int) else (index + step) % count
    return index ^ step


def relative(owner, me, count):
    if count & (count - 1):
        return lax.rem(owner - me + count, count)
    return owner ^ me


def plan_kernel(groups, half, slot_ref, owner_ref, select_ref):
    subarrays = slot_ref.shape[0]
    blocks = owner_ref.shape[0]
    per = subarrays // groups
    me = lax.axis_index("tm")
    shape = (subarrays, LANES)
    place = lax.broadcasted_iota(jnp.int32, shape, 0)
    name = jnp.zeros(shape, jnp.int32)
    for s in range(subarrays):
        name = jnp.where(place == s, slot_ref[s], name)
    base = jnp.zeros(shape, jnp.int32)
    for s in range(subarrays):
        chunk = relative(jnp.int32(s // per), me, groups) * per + s % per
        base = jnp.where(place == s, chunk * half, base)
    base = base.astype(jnp.float32)
    earlier = lax.broadcasted_iota(jnp.int32, (LANES, LANES), 0)
    later = lax.broadcasted_iota(jnp.int32, (LANES, LANES), 1)
    before = jnp.where(earlier < later, 1.0, 0.0).astype(jnp.bfloat16)
    held = [jnp.where(owner_ref[b : b + 1, :] == name, 1.0, 0.0) for b in range(blocks)]
    within = jnp.dot(
        jnp.concatenate(held, axis=0).astype(jnp.bfloat16), before, preferred_element_type=jnp.float32
    )
    run = base
    height = 256
    row = lax.broadcasted_iota(jnp.int32, (height, LANES), 0).astype(jnp.float32)
    for b in range(blocks):
        rank = within[b * subarrays : (b + 1) * subarrays] + run
        target = jnp.sum(held[b] * rank, axis=0, keepdims=True)
        run = run + jnp.sum(held[b], axis=1, keepdims=True)
        for top in range(0, select_ref.shape[0], height):
            hit = row == (target - top)
            select_ref[top : top + height, b * LANES : (b + 1) * LANES] = jnp.where(hit, 1.0, 0.0).astype(
                jnp.bfloat16
            )


def plan(assignment, slot_subarray_index, groups, half):
    antennas = assignment.shape[0]
    subarrays = slot_subarray_index.shape[0]
    return pl.pallas_call(
        functools.partial(plan_kernel, groups, half),
        out_shape=jax.ShapeDtypeStruct((subarrays * half, antennas), jnp.bfloat16),
        in_specs=[SMEM, VMEM],
        out_specs=VMEM,
        compiler_params=PARAMS,
        cost_estimate=pl.CostEstimate(flops=4_000_000_000, bytes_accessed=3_000_000, transcendentals=0),
    )(slot_subarray_index, assignment.reshape(antennas // LANES, LANES))


def gather_kernel(select_ref, x_ref, *rest):
    *outs, wide, pair, tall = rest
    inputs = x_ref.shape[0]
    antennas = inputs // 2
    wide[...] = x_ref[...].astype(jnp.float32)
    for pol in range(2):
        pair[:, pol * LANES : (pol + 1) * LANES] = wide[pl.ds(pol, antennas, stride=2), :].astype(jnp.bfloat16)
    picked = jnp.dot(select_ref[...], pair[...], preferred_element_type=jnp.float32)
    rows = select_ref.shape[0]
    for pol in range(2):
        tall[pl.ds(pol, rows, stride=2), :] = picked[:, pol * LANES : (pol + 1) * LANES]
    per, slots, _ = outs[0].shape
    for g, out in enumerate(outs):
        for s in range(per):
            top = (g * per + s) * slots
            out[s] = tall[top : top + slots, :].astype(jnp.bfloat16)


def gather(select, x, groups, per, slots):
    inputs, samples = x.shape
    rows, antennas = select.shape
    return pl.pallas_call(
        gather_kernel,
        out_shape=[jax.ShapeDtypeStruct((per, slots, samples), jnp.bfloat16)] * groups,
        in_specs=[VMEM, VMEM],
        out_specs=[VMEM] * groups,
        scratch_shapes=[
            pltpu.VMEM((inputs, samples), jnp.float32),
            pltpu.VMEM((antennas, 2 * samples), jnp.bfloat16),
            pltpu.VMEM((2 * rows, samples), jnp.float32),
        ],
        compiler_params=PARAMS,
        cost_estimate=pl.CostEstimate(
            flops=2 * rows * antennas * 2 * samples, bytes_accessed=4_000_000, transcendentals=0
        ),
    )(select, x)


def gram_kernel(*refs):
    *parts, out = refs
    count = len(parts) // 2
    for s in range(parts[0].shape[0]):
        for part in range(2):
            total = None
            for e in range(count):
                real, imag = parts[e][s], parts[count + e][s]
                right = jnp.concatenate([real, imag], axis=1)
                left = right if part == 0 else jnp.concatenate([imag, -real], axis=1)
                term = lax.dot_general(
                    left, right, (((1,), (1,)), ((), ())), preferred_element_type=jnp.float32
                )
                total = term if total is None else total + term
            out[s, 0, part] = total


def gram(real, imag):
    per, slots, _ = real[0].shape
    return pl.pallas_call(
        gram_kernel,
        out_shape=jax.ShapeDtypeStruct((per, 1, 2, slots, slots), jnp.float32),
        in_specs=[VMEM] * (2 * len(real)),
        out_specs=VMEM,
        compiler_params=PARAMS,
        cost_estimate=pl.CostEstimate(flops=1_200_000_000, bytes_accessed=4_000_000, transcendentals=0),
    )(*real, *imag)


def shards(voltages, assignment, slot_subarray_index):
    groups = lax.axis_size("tm")
    subarrays = slot_subarray_index.shape[0]
    per = subarrays // groups
    select = plan(assignment, slot_subarray_index, groups, SLOT // 2)
    order = sorted(range(1, groups), reverse=True)
    received = []
    for k in range(2):
        x = lax.all_to_all(voltages[k], "chan", split_axis=0, concat_axis=1, tiled=True)
        x = x.reshape(x.shape[1], x.shape[2])
        chunks = gather(select, x, groups, per, SLOT)
        got = [chunks[0]] + [None] * (groups - 1)
        for step in order:
            pairs = [(j, partner(j, step, groups)) for j in range(groups)]
            got[step] = lax.ppermute(chunks[step], "tm", pairs)
        received.append(got)
    return gram(received[0], received[1])


def solution(mesh):
    placed = (P(None, None, "chan", "tm"), P(), P())
    return jax.shard_map(
        shards,
        mesh=mesh,
        in_specs=placed,
        out_specs=P("tm", "chan", None, None, None),
        check_vma=False,
    )
```

```python
import functools

import jax
import jax.numpy as jnp
from jax import lax
from jax.experimental import pallas as pl
from jax.experimental.pallas import tpu as pltpu
from jax.sharding import PartitionSpec as P


SLOT = 384
LANES = 128

VMEM = pl.BlockSpec(memory_space=pltpu.VMEM)
SMEM = pl.BlockSpec(memory_space=pltpu.SMEM)
PARAMS = pltpu.CompilerParams(vmem_limit_bytes=20 * 1024 * 1024)


def partner(index, step, count):
    if count & (count - 1):
        return lax.rem(index + step, count) if not isinstance(index, int) else (index + step) % count
    return index ^ step


def relative(owner, me, count):
    if count & (count - 1):
        return lax.rem(owner - me + count, count)
    return owner ^ me


def plan_kernel(groups, half, slot_ref, owner_ref, select_ref):
    subarrays = slot_ref.shape[0]
    blocks = owner_ref.shape[0]
    per = subarrays // groups
    me = lax.axis_index("tm")
    shape = (subarrays, LANES)
    place = lax.broadcasted_iota(jnp.int32, shape, 0)
    name = jnp.zeros(shape, jnp.int32)
    for s in range(subarrays):
        name = jnp.where(place == s, slot_ref[s], name)
    base = jnp.zeros(shape, jnp.int32)
    for s in range(subarrays):
        chunk = relative(jnp.int32(s // per), me, groups) * per + s % per
        base = jnp.where(place == s, chunk * half, base)
    base = base.astype(jnp.float32)
    earlier = lax.broadcasted_iota(jnp.int32, (LANES, LANES), 0)
    later = lax.broadcasted_iota(jnp.int32, (LANES, LANES), 1)
    before = jnp.where(earlier < later, 1.0, 0.0).astype(jnp.bfloat16)
    held = [jnp.where(owner_ref[b : b + 1, :] == name, 1.0, 0.0) for b in range(blocks)]
    within = jnp.dot(
        jnp.concatenate(held, axis=0).astype(jnp.bfloat16), before, preferred_element_type=jnp.float32
    )
    run = base
    height = 256
    row = lax.broadcasted_iota(jnp.int32, (height, LANES), 0).astype(jnp.float32)
    for b in range(blocks):
        rank = within[b * subarrays : (b + 1) * subarrays] + run
        target = jnp.sum(held[b] * rank, axis=0, keepdims=True)
        run = run + jnp.sum(held[b], axis=1, keepdims=True)
        for top in range(0, select_ref.shape[0], height):
            hit = row == (target - top)
            select_ref[top : top + height, b * LANES : (b + 1) * LANES] = jnp.where(hit, 1.0, 0.0).astype(
                jnp.bfloat16
            )


def plan(assignment, slot_subarray_index, groups, half):
    antennas = assignment.shape[0]
    subarrays = slot_subarray_index.shape[0]
    return pl.pallas_call(
        functools.partial(plan_kernel, groups, half),
        out_shape=jax.ShapeDtypeStruct((subarrays * half, antennas), jnp.bfloat16),
        in_specs=[SMEM, VMEM],
        out_specs=VMEM,
        compiler_params=PARAMS,
        cost_estimate=pl.CostEstimate(flops=4_000_000_000, bytes_accessed=3_000_000, transcendentals=0),
    )(slot_subarray_index, assignment.reshape(antennas // LANES, LANES))


def split_kernel(steps, x_ref, *rest):
    *outs, sem = rest
    chunks, other = outs[:-1], outs[-1]
    me = lax.axis_index("chan")
    copies = [
        pltpu.make_async_copy(x_ref.at[0, partner(me, step, len(steps))], chunk, sem.at[i])
        for i, (step, chunk) in enumerate(zip(steps, chunks))
    ]
    copies.append(pltpu.make_async_copy(x_ref.at[1], other, sem.at[len(steps)]))
    for copy in copies:
        copy.start()
    for copy in copies:
        copy.wait()


def split(voltages, steps):
    _, chans, inputs, samples = voltages.shape
    piece = jax.ShapeDtypeStruct((inputs, samples), voltages.dtype)
    return pl.pallas_call(
        functools.partial(split_kernel, steps),
        out_shape=[piece] * len(steps) + [jax.ShapeDtypeStruct((chans, inputs, samples), voltages.dtype)],
        in_specs=[pl.BlockSpec(memory_space=pltpu.HBM)],
        out_specs=[VMEM] * (len(steps) + 1),
        scratch_shapes=[pltpu.SemaphoreType.DMA((len(steps) + 1,))],
        compiler_params=PARAMS,
        cost_estimate=pl.CostEstimate(flops=1_000_000, bytes_accessed=2_000_000, transcendentals=0),
    )(voltages)


def gather_kernel(steps, outputs, select_ref, *rest):
    xs, outs = rest[: len(steps)], rest[len(steps) : len(steps) + outputs]
    wide, pair, tall = rest[len(steps) + outputs :]
    inputs = xs[0].shape[0]
    antennas = inputs // 2
    me = lax.axis_index("chan")
    for i, (step, x) in enumerate(zip(steps, xs)):
        wide[i * inputs : (i + 1) * inputs] = x[...].astype(jnp.float32)
        if len(steps) == 1:
            top = 0
        else:
            top = pl.multiple_of(partner(me, step, len(steps)) * antennas, antennas)
        for pol in range(2):
            pair[pl.ds(top, antennas), pol * LANES : (pol + 1) * LANES] = wide[
                pl.ds(i * inputs + pol, antennas, stride=2), :
            ].astype(jnp.bfloat16)
    picked = jnp.dot(select_ref[...], pair[...], preferred_element_type=jnp.float32)
    rows = select_ref.shape[0]
    for pol in range(2):
        tall[pl.ds(pol, rows, stride=2), :] = picked[:, pol * LANES : (pol + 1) * LANES]
    per, slots, _ = outs[0].shape
    for g, out in enumerate(outs):
        for s in range(per):
            top = (g * per + s) * slots
            out[s] = tall[top : top + slots, :].astype(jnp.bfloat16)


def gather(select, xs, steps, groups, per, slots):
    _, samples = xs[0].shape
    rows, antennas = select.shape
    return pl.pallas_call(
        functools.partial(gather_kernel, steps, groups),
        out_shape=[jax.ShapeDtypeStruct((per, slots, samples), jnp.bfloat16)] * groups,
        in_specs=[VMEM] * (1 + len(xs)),
        out_specs=[VMEM] * groups,
        scratch_shapes=[
            pltpu.VMEM((2 * antennas, samples), jnp.float32),
            pltpu.VMEM((antennas, 2 * samples), jnp.bfloat16),
            pltpu.VMEM((2 * rows, samples), jnp.float32),
        ],
        compiler_params=PARAMS,
        cost_estimate=pl.CostEstimate(
            flops=2 * rows * antennas * 2 * samples, bytes_accessed=4_000_000, transcendentals=0
        ),
    )(select, *xs)


def products(real, imag, part):
    right = jnp.concatenate([real, imag], axis=1)
    left = right if part == 0 else jnp.concatenate([imag, -real], axis=1)
    return lax.dot_general(left, right, (((1,), (1,)), ((), ())), preferred_element_type=jnp.float32)


def early_kernel(*refs):
    *parts, out = refs
    count = len(parts) // 2
    for s in range(parts[0].shape[0]):
        for part in range(2):
            total = None
            for e in range(count):
                term = products(parts[e][s], parts[count + e][s], part)
                total = term if total is None else total + term
            out[s, part] = total


def late_kernel(real, imag, so_far, out, stage, sem):
    copies = []
    for s in range(real.shape[0]):
        for part in range(2):
            stage[s, part] = so_far[s, part] + products(real[s], imag[s], part)
            copy = pltpu.make_async_copy(stage.at[s, part], out.at[s, 0, part], sem.at[s, part])
            copy.start()
            copies.append(copy)
    for copy in copies:
        copy.wait()


def gram(real, imag, last):
    per, slots, samples = real[0].shape
    early = [e for e in range(len(real)) if e != last]
    flops = 2 * per * 2 * slots * slots * 2 * samples
    so_far = pl.pallas_call(
        early_kernel,
        out_shape=jax.ShapeDtypeStruct((per, 2, slots, slots), jnp.float32),
        in_specs=[VMEM] * (2 * len(early)),
        out_specs=VMEM,
        compiler_params=PARAMS,
        cost_estimate=pl.CostEstimate(flops=flops * len(early), bytes_accessed=3_000_000, transcendentals=0),
    )(*[real[e] for e in early], *[imag[e] for e in early])
    return pl.pallas_call(
        late_kernel,
        out_shape=jax.ShapeDtypeStruct((per, 1, 2, slots, slots), jnp.float32),
        in_specs=[VMEM] * 3,
        out_specs=pl.BlockSpec(memory_space=pl.ANY),
        scratch_shapes=[
            pltpu.VMEM((per, 2, slots, slots), jnp.float32),
            pltpu.SemaphoreType.DMA((per, 2)),
        ],
        compiler_params=PARAMS,
        cost_estimate=pl.CostEstimate(flops=flops, bytes_accessed=3_000_000, transcendentals=0),
    )(real[last], imag[last], so_far)


def exchange(chunks, order, groups):
    got = list(chunks)
    for step in order:
        pairs = [(j, partner(j, step, groups)) for j in range(groups)]
        got[step] = lax.ppermute(chunks[step], "tm", pairs)
    return got


def across(x):
    x = lax.all_to_all(x, "chan", split_axis=0, concat_axis=1, tiled=True)
    return x.reshape(x.shape[1], x.shape[2])


def steps_of(voltages, assignment, slot_subarray_index):
    groups = lax.axis_size("tm")
    chans = lax.axis_size("chan")
    subarrays = slot_subarray_index.shape[0]
    per = subarrays // groups
    order = sorted(range(1, groups), reverse=True)
    last = order[0]
    if chans <= 8 and chans & (chans - 1) == 0:
        steps = tuple(range(chans))
        *chunks, imag = split(voltages, steps)
        reals = list(chunks)
        for step in (6, 7, 2, 3, 4, 5, 1):
            if step < chans:
                pairs = [(j, j ^ step) for j in range(chans)]
                reals[step] = lax.ppermute(chunks[step], "chan", pairs)
    else:
        steps, imag = (0,), voltages[1]
        reals = [across(voltages[0])]
    select = plan(assignment, slot_subarray_index, groups, SLOT // 2)
    real = exchange(gather(select, reals, steps, groups, per, SLOT), order, groups)
    imag = across(imag)
    imag = exchange(gather(select, [imag], (0,), groups, per, SLOT), order[1:] + order[:1], groups)
    return gram(real, imag, last)


def solution(mesh):
    placed = (P(None, None, "chan", "tm"), P(), P())
    return jax.shard_map(
        steps_of,
        mesh=mesh,
        in_specs=placed,
        out_specs=P("tm", "chan", None, None, None),
        check_vma=False,
    )
```

```python
import functools

import jax
import jax.numpy as jnp
from jax import lax
from jax.experimental import pallas as pl
from jax.experimental.pallas import tpu as pltpu
from jax.sharding import PartitionSpec as P


SLOT = 384
LANES = 128


VMEM = pl.BlockSpec(memory_space=pltpu.VMEM)
SMEM = pl.BlockSpec(memory_space=pltpu.SMEM)
PARAMS = pltpu.CompilerParams(vmem_limit_bytes=20 * 1024 * 1024)


def partner(index, step, count):
    if count & (count - 1):
        return lax.rem(index + step, count) if not isinstance(index, int) else (index + step) % count
    return index ^ step


def relative(owner, me, count):
    if count & (count - 1):
        return lax.rem(owner - me + count, count)
    return owner ^ me


def plan_kernel(groups, half, slot_ref, owner_ref, select_ref):
    subarrays = slot_ref.shape[0]
    blocks = owner_ref.shape[0]
    per = subarrays // groups
    me = lax.axis_index("tm")
    shape = (subarrays, LANES)
    place = lax.broadcasted_iota(jnp.int32, shape, 0)
    name = jnp.zeros(shape, jnp.int32)
    for s in range(subarrays):
        name = jnp.where(place == s, slot_ref[s], name)
    base = jnp.zeros(shape, jnp.int32)
    for s in range(subarrays):
        chunk = relative(jnp.int32(s // per), me, groups) * per + s % per
        base = jnp.where(place == s, chunk * half, base)
    base = base.astype(jnp.float32)
    earlier = lax.broadcasted_iota(jnp.int32, (LANES, LANES), 0)
    later = lax.broadcasted_iota(jnp.int32, (LANES, LANES), 1)
    before = jnp.where(earlier < later, 1.0, 0.0).astype(jnp.bfloat16)
    held = [jnp.where(owner_ref[b : b + 1, :] == name, 1.0, 0.0) for b in range(blocks)]
    within = jnp.dot(
        jnp.concatenate(held, axis=0).astype(jnp.bfloat16), before, preferred_element_type=jnp.float32
    )
    run = base
    height = 256
    row = lax.broadcasted_iota(jnp.int32, (height, LANES), 0).astype(jnp.float32)
    for b in range(blocks):
        rank = within[b * subarrays : (b + 1) * subarrays] + run
        target = jnp.sum(held[b] * rank, axis=0, keepdims=True)
        run = run + jnp.sum(held[b], axis=1, keepdims=True)
        for top in range(0, select_ref.shape[0], height):
            hit = row == (target - top)
            select_ref[top : top + height, b * LANES : (b + 1) * LANES] = jnp.where(hit, 1.0, 0.0).astype(
                jnp.bfloat16
            )


def plan(assignment, slot_subarray_index, groups, half):
    antennas = assignment.shape[0]
    subarrays = slot_subarray_index.shape[0]
    return pl.pallas_call(
        functools.partial(plan_kernel, groups, half),
        out_shape=jax.ShapeDtypeStruct((subarrays * half, antennas), jnp.bfloat16),
        in_specs=[SMEM, VMEM],
        out_specs=VMEM,
        compiler_params=PARAMS,
        cost_estimate=pl.CostEstimate(flops=4_000_000_000, bytes_accessed=3_000_000, transcendentals=0),
    )(slot_subarray_index, assignment.reshape(antennas // LANES, LANES))


def split_kernel(chans, x_ref, *rest):
    *outs, sem = rest
    me = lax.axis_index("chan")
    early = chans // 2
    wanted = [(x_ref.at[1, me ^ (2 * r + (me & 1))], outs[0].at[r]) for r in range(early)]
    for k in range(2):
        wanted += [(x_ref.at[k, me ^ s], outs[1 + k * chans + s]) for s in range(chans)]
    copies = [pltpu.make_async_copy(a, b, sem.at[i]) for i, (a, b) in enumerate(wanted)]
    for copy in copies:
        copy.start()
    for copy in copies:
        copy.wait()


def split(voltages):
    _, chans, inputs, samples = voltages.shape
    piece = jax.ShapeDtypeStruct((inputs, samples), voltages.dtype)
    raw = jax.ShapeDtypeStruct((chans // 2, inputs, samples), voltages.dtype)
    out = pl.pallas_call(
        functools.partial(split_kernel, chans),
        out_shape=[raw] + [piece] * (2 * chans),
        in_specs=[pl.BlockSpec(memory_space=pltpu.HBM)],
        out_specs=[VMEM] * (2 * chans + 1),
        scratch_shapes=[pltpu.SemaphoreType.DMA((2 * chans + chans // 2,))],
        compiler_params=PARAMS,
        cost_estimate=pl.CostEstimate(flops=1_000_000, bytes_accessed=2_000_000, transcendentals=0),
    )(voltages)
    return out[0], out[1 : 1 + chans], out[1 + chans :]


def unstack_kernel(x_ref, *outs):
    for r, out in enumerate(outs):
        out[...] = x_ref[r]


def unstack(x):
    count, inputs, samples = x.shape
    return pl.pallas_call(
        unstack_kernel,
        out_shape=[jax.ShapeDtypeStruct((inputs, samples), x.dtype)] * count,
        in_specs=[VMEM],
        out_specs=[VMEM] * count,
        compiler_params=PARAMS,
        cost_estimate=pl.CostEstimate(flops=1_000_000, bytes_accessed=500_000, transcendentals=0),
    )(x)


def load_pair(steps, xs, wide, pair):
    inputs = xs[0].shape[0]
    antennas = inputs // 2
    me = lax.axis_index("chan")
    for i, (step, x) in enumerate(zip(steps, xs)):
        wide[i * inputs : (i + 1) * inputs] = x[...].astype(jnp.float32)
        if len(steps) == 1:
            top = 0
        else:
            top = pl.multiple_of(partner(me, step, len(steps)) * antennas, antennas)
        for pol in range(2):
            pair[pl.ds(top, antennas), pol * LANES : (pol + 1) * LANES] = wide[
                pl.ds(i * inputs + pol, antennas, stride=2), :
            ].astype(jnp.bfloat16)


def store_rows(picked, tall, outs):
    rows = picked.shape[0]
    for pol in range(2):
        tall[pl.ds(pol, rows, stride=2), :] = picked[:, pol * LANES : (pol + 1) * LANES]
    per, slots, _ = outs[0].shape
    for g, out in enumerate(outs):
        for s in range(per):
            top = (g * per + s) * slots
            out[s] = tall[top : top + slots, :].astype(jnp.bfloat16)


def gather_kernel(steps, outputs, select_ref, *rest):
    xs, outs = rest[: len(steps)], rest[len(steps) : len(steps) + outputs]
    wide, pair, tall = rest[len(steps) + outputs :]
    load_pair(steps, xs, wide, pair)
    picked = jnp.dot(select_ref[...], pair[...], preferred_element_type=jnp.float32)
    store_rows(picked, tall, outs)


def twin_kernel(steps, select_ref, *rest):
    count = len(steps)
    own, other = rest[:count], rest[count : 2 * count]
    outs = rest[2 * count : 2 * count + 4]
    wide, pair, tall = rest[2 * count + 4 :]
    odd = lax.axis_index("chan") & 1
    rows = select_ref.shape[0] // 2
    load_pair(steps, own, wide.at[0], pair.at[0])
    picked = jnp.dot(select_ref[:rows], pair[0], preferred_element_type=jnp.float32)
    store_rows(picked, tall.at[0], outs[:2])
    load_pair(steps, other, wide.at[1], pair.at[1])
    top = pl.multiple_of(odd * rows, rows)
    picked = jnp.dot(select_ref[pl.ds(top, rows)], pair[1 - odd], preferred_element_type=jnp.float32)
    store_rows(picked, tall.at[1], outs[2:])


def twin(select, own, other, steps, per, slots):
    _, samples = own[0].shape
    rows, antennas = select.shape
    return pl.pallas_call(
        functools.partial(twin_kernel, steps),
        out_shape=[jax.ShapeDtypeStruct((per, slots, samples), jnp.bfloat16)] * 4,
        in_specs=[VMEM] * (1 + 2 * len(own)),
        out_specs=[VMEM] * 4,
        scratch_shapes=[
            pltpu.VMEM((2, 2 * antennas, samples), jnp.float32),
            pltpu.VMEM((2, antennas, 2 * samples), jnp.bfloat16),
            pltpu.VMEM((2, rows, samples), jnp.float32),
        ],
        compiler_params=PARAMS,
        cost_estimate=pl.CostEstimate(
            flops=2 * rows * antennas * 2 * samples, bytes_accessed=4_000_000, transcendentals=0
        ),
    )(select, *own, *other)


def gather(select, xs, steps, groups, per, slots):
    _, samples = xs[0].shape
    rows, antennas = select.shape
    return pl.pallas_call(
        functools.partial(gather_kernel, steps, groups),
        out_shape=[jax.ShapeDtypeStruct((per, slots, samples), jnp.bfloat16)] * groups,
        in_specs=[VMEM] * (1 + len(xs)),
        out_specs=[VMEM] * groups,
        scratch_shapes=[
            pltpu.VMEM((2 * antennas, samples), jnp.float32),
            pltpu.VMEM((antennas, 2 * samples), jnp.bfloat16),
            pltpu.VMEM((2 * rows, samples), jnp.float32),
        ],
        compiler_params=PARAMS,
        cost_estimate=pl.CostEstimate(
            flops=2 * rows * antennas * 2 * samples, bytes_accessed=4_000_000, transcendentals=0
        ),
    )(select, *xs)


def products(real, imag, part):
    right = jnp.concatenate([real, imag], axis=1)
    left = right if part == 0 else jnp.concatenate([imag, -real], axis=1)
    return lax.dot_general(left, right, (((1,), (1,)), ((), ())), preferred_element_type=jnp.float32)


def early_kernel(*refs):
    *parts, out = refs
    count = len(parts) // 2
    for s in range(parts[0].shape[0]):
        for part in range(2):
            total = None
            for e in range(count):
                term = products(parts[e][s], parts[count + e][s], part)
                total = term if total is None else total + term
            out[s, part] = total


def late_kernel(real, *rest):
    *imags, so_far, out, stage, sem = rest
    slots, samples = real.shape[1:]
    odd = lax.axis_index("chan") & 1
    copies = []
    for s in range(real.shape[0]):
        imag = imags[0][s]
        if len(imags) == 2:
            imag = jnp.where(jnp.full((slots, samples), odd) == 1, imags[1][s].astype(jnp.float32), imag.astype(jnp.float32))
            imag = imag.astype(jnp.bfloat16)
        for part in range(2):
            stage[s, part] = so_far[s, part] + products(real[s], imag, part)
            copy = pltpu.make_async_copy(stage.at[s, part], out.at[s, 0, part], sem.at[s, part])
            copy.start()
            copies.append(copy)
    for copy in copies:
        copy.wait()


def gram(real, imag, last):
    per, slots, samples = real[0].shape
    early = [e for e in range(len(real)) if e != last]
    ends = imag[last] if isinstance(imag[last], tuple) else (imag[last],)
    flops = 2 * per * 2 * slots * slots * 2 * samples
    so_far = pl.pallas_call(
        early_kernel,
        out_shape=jax.ShapeDtypeStruct((per, 2, slots, slots), jnp.float32),
        in_specs=[VMEM] * (2 * len(early)),
        out_specs=VMEM,
        compiler_params=PARAMS,
        cost_estimate=pl.CostEstimate(flops=flops * len(early), bytes_accessed=3_000_000, transcendentals=0),
    )(*[real[e] for e in early], *[imag[e] for e in early])
    return pl.pallas_call(
        late_kernel,
        out_shape=jax.ShapeDtypeStruct((per, 1, 2, slots, slots), jnp.float32),
        in_specs=[VMEM] * (2 + len(ends)),
        out_specs=pl.BlockSpec(memory_space=pl.ANY),
        scratch_shapes=[
            pltpu.VMEM((per, 2, slots, slots), jnp.float32),
            pltpu.SemaphoreType.DMA((per, 2)),
        ],
        compiler_params=PARAMS,
        cost_estimate=pl.CostEstimate(flops=flops, bytes_accessed=3_000_000, transcendentals=0),
    )(real[last], *ends, so_far)


def exchange(chunks, order, groups):
    got = list(chunks)
    for step in order:
        pairs = [(j, partner(j, step, groups)) for j in range(groups)]
        got[step] = lax.ppermute(chunks[step], "tm", pairs)
    return got


def across(x):
    x = lax.all_to_all(x, "chan", split_axis=0, concat_axis=1, tiled=True)
    return x.reshape(x.shape[1], x.shape[2])


CHAN_ORDER = (6, 7, 2, 3, 4, 5, 1)


def cross(chunks, chans):
    got = list(chunks)
    for step in CHAN_ORDER:
        if step < chans:
            got[step] = lax.ppermute(chunks[step], "chan", [(i, i ^ step) for i in range(chans)])
    return got


def paired(chans, groups):
    return groups == 4 and chans in (2, 4, 8)


def steps_of(voltages, assignment, slot_subarray_index):
    groups = lax.axis_size("tm")
    chans = lax.axis_size("chan")
    subarrays = slot_subarray_index.shape[0]
    per = subarrays // groups
    order = sorted(range(1, groups), reverse=True)
    last = 2 if groups == 4 else order[0]
    first = [step for step in order if step != last]
    if not paired(chans, groups):
        select = plan(assignment, slot_subarray_index, groups, SLOT // 2)
        real = across(voltages[0])
        real = exchange(gather(select, [real], (0,), groups, per, SLOT), order, groups)
        imag = across(voltages[1])
        imag = exchange(gather(select, [imag], (0,), groups, per, SLOT), first + [last], groups)
        return gram(real, imag, last)

    steps = tuple(range(chans))
    device = [(i, j, i * groups + j) for i in range(chans) for j in range(groups)]
    raw, reals, imags = split(voltages)
    raw = lax.ppermute(raw, "tm", [(j, j ^ 2) for j in range(groups)])
    reals = cross(reals, chans)
    select = plan(assignment, slot_subarray_index, groups, SLOT // 2)
    real = exchange(gather(select, reals, steps, groups, per, SLOT), order, groups)

    imags = cross(imags, chans)
    pieces = unstack(raw)
    far = [pieces[s // 2] for s in steps]
    for step in CHAN_ORDER:
        if step < chans:
            pairs = [(i, i ^ step) for i in range(chans) if (i ^ step) % 2 == 0]
            far[step] = lax.ppermute(far[step], "chan", pairs)
    mine, near, third, fourth = twin(select, imags, far, steps, per, SLOT)
    pairs = [(n, i * groups + (j ^ (3 if i % 2 else 1))) for i, j, n in device]
    fourth = lax.ppermute(fourth, ("chan", "tm"), pairs)
    pairs = [(n, i * groups + (j ^ 2)) for i, j, n in device if i % 2]
    there = lax.ppermute(third, ("chan", "tm"), pairs)
    near = lax.ppermute(near, "tm", [(j, j ^ 1) for j in range(groups)])
    return gram(real, [mine, near, (third, there), fourth], last)


def solution(mesh):
    placed = (P(None, None, "chan", "tm"), P(), P())
    return jax.shard_map(
        steps_of,
        mesh=mesh,
        in_specs=placed,
        out_specs=P("tm", "chan", None, None, None),
        check_vma=False,
    )
```

```python
import functools

import jax
import jax.numpy as jnp
from jax import lax
from jax.experimental import pallas as pl
from jax.experimental.pallas import tpu as pltpu
from jax.sharding import PartitionSpec as P


SLOT = 384
LANES = 128


VMEM = pl.BlockSpec(memory_space=pltpu.VMEM)
SMEM = pl.BlockSpec(memory_space=pltpu.SMEM)
PARAMS = pltpu.CompilerParams(vmem_limit_bytes=20 * 1024 * 1024)


def partner(index, step, count):
    if count & (count - 1):
        return lax.rem(index + step, count) if not isinstance(index, int) else (index + step) % count
    return index ^ step


def relative(owner, me, count):
    if count & (count - 1):
        return lax.rem(owner - me + count, count)
    return owner ^ me


def plan_kernel(groups, half, slot_ref, owner_ref, select_ref):
    subarrays = slot_ref.shape[0]
    blocks = owner_ref.shape[0]
    per = subarrays // groups
    me = lax.axis_index("tm")
    shape = (subarrays, LANES)
    place = lax.broadcasted_iota(jnp.int32, shape, 0)
    name = jnp.zeros(shape, jnp.int32)
    for s in range(subarrays):
        name = jnp.where(place == s, slot_ref[s], name)
    base = jnp.zeros(shape, jnp.int32)
    for s in range(subarrays):
        chunk = relative(jnp.int32(s // per), me, groups) * per + s % per
        base = jnp.where(place == s, chunk * half, base)
    base = base.astype(jnp.float32)
    earlier = lax.broadcasted_iota(jnp.int32, (LANES, LANES), 0)
    later = lax.broadcasted_iota(jnp.int32, (LANES, LANES), 1)
    before = jnp.where(earlier < later, 1.0, 0.0).astype(jnp.bfloat16)
    held = [jnp.where(owner_ref[b : b + 1, :] == name, 1.0, 0.0) for b in range(blocks)]
    within = jnp.dot(
        jnp.concatenate(held, axis=0).astype(jnp.bfloat16), before, preferred_element_type=jnp.float32
    )
    run = base
    height = 256
    row = lax.broadcasted_iota(jnp.int32, (height, LANES), 0).astype(jnp.float32)
    for b in range(blocks):
        rank = within[b * subarrays : (b + 1) * subarrays] + run
        target = jnp.sum(held[b] * rank, axis=0, keepdims=True)
        run = run + jnp.sum(held[b], axis=1, keepdims=True)
        for top in range(0, select_ref.shape[0], height):
            hit = row == (target - top)
            select_ref[top : top + height, b * LANES : (b + 1) * LANES] = jnp.where(hit, 1.0, 0.0).astype(
                jnp.bfloat16
            )


def plan(assignment, slot_subarray_index, groups, half):
    antennas = assignment.shape[0]
    subarrays = slot_subarray_index.shape[0]
    return pl.pallas_call(
        functools.partial(plan_kernel, groups, half),
        out_shape=jax.ShapeDtypeStruct((subarrays * half, antennas), jnp.bfloat16),
        in_specs=[SMEM, VMEM],
        out_specs=VMEM,
        compiler_params=PARAMS,
        cost_estimate=pl.CostEstimate(flops=4_000_000_000, bytes_accessed=3_000_000, transcendentals=0),
    )(slot_subarray_index, assignment.reshape(antennas // LANES, LANES))


def give_kernel(chips, x_ref, out):
    me = lax.axis_index("chan")
    for k in range(2):
        for t in range(chips):
            out[k, t] = x_ref[k, (me ^ (2 * t)) ^ 1]


def give(voltages):
    parts, chans, inputs, samples = voltages.shape
    return pl.pallas_call(
        functools.partial(give_kernel, chans // 2),
        out_shape=jax.ShapeDtypeStruct((parts, chans // 2, inputs, samples), voltages.dtype),
        in_specs=[VMEM],
        out_specs=VMEM,
        compiler_params=PARAMS,
        cost_estimate=pl.CostEstimate(flops=1_000_000, bytes_accessed=1_000_000, transcendentals=0),
    )(voltages)


def merge_kernel(chips, x_ref, given_ref, raw, *outs):
    me = lax.axis_index("chan")
    inputs = x_ref.shape[2]
    mine = pl.multiple_of((me & 1) * inputs, inputs)
    theirs = pl.multiple_of(inputs - (me & 1) * inputs, inputs)
    for k in range(2):
        for t in range(chips):
            out = outs[k * chips + t]
            piece, other = x_ref[k, me ^ (2 * t)], given_ref[k, t]
            out[pl.ds(mine, inputs)] = piece
            out[pl.ds(theirs, inputs)] = other
            if k:
                raw[t, pl.ds(mine, inputs)] = piece
                raw[t, pl.ds(theirs, inputs)] = other


def merge(voltages, given):
    parts, chans, inputs, samples = voltages.shape
    chips = chans // 2
    piece = jax.ShapeDtypeStruct((2 * inputs, samples), voltages.dtype)
    raw = jax.ShapeDtypeStruct((chips, 2 * inputs, samples), voltages.dtype)
    out = pl.pallas_call(
        functools.partial(merge_kernel, chips),
        out_shape=[raw] + [piece] * (parts * chips),
        in_specs=[VMEM] * 2,
        out_specs=[VMEM] * (1 + parts * chips),
        compiler_params=PARAMS,
        cost_estimate=pl.CostEstimate(flops=1_000_000, bytes_accessed=2_000_000, transcendentals=0),
    )(voltages, given)
    return out[0], out[1 : 1 + chips], out[1 + chips :]


def unstack_kernel(x_ref, *outs):
    for r, out in enumerate(outs):
        out[...] = x_ref[r]


def unstack(x):
    count, inputs, samples = x.shape
    return pl.pallas_call(
        unstack_kernel,
        out_shape=[jax.ShapeDtypeStruct((inputs, samples), x.dtype)] * count,
        in_specs=[VMEM],
        out_specs=[VMEM] * count,
        compiler_params=PARAMS,
        cost_estimate=pl.CostEstimate(flops=1_000_000, bytes_accessed=500_000, transcendentals=0),
    )(x)


def load_pair(steps, xs, wide, pair):
    inputs = xs[0].shape[0]
    antennas = inputs // 2
    chip = lax.axis_index("chan") // 2
    for i, (step, x) in enumerate(zip(steps, xs)):
        wide[i * inputs : (i + 1) * inputs] = x[...].astype(jnp.float32)
        if len(steps) == 1:
            top = 0
        else:
            top = pl.multiple_of((chip ^ step) * antennas, antennas)
        for pol in range(2):
            pair[pl.ds(top, antennas), pol * LANES : (pol + 1) * LANES] = wide[
                pl.ds(i * inputs + pol, antennas, stride=2), :
            ].astype(jnp.bfloat16)


def store_rows(picked, tall, outs):
    rows = picked.shape[0]
    for pol in range(2):
        tall[pl.ds(pol, rows, stride=2), :] = picked[:, pol * LANES : (pol + 1) * LANES]
    per, slots, _ = outs[0].shape
    for g, out in enumerate(outs):
        for s in range(per):
            top = (g * per + s) * slots
            out[s] = tall[top : top + slots, :].astype(jnp.bfloat16)


def gather_kernel(steps, outputs, select_ref, *rest):
    xs, outs = rest[: len(steps)], rest[len(steps) : len(steps) + outputs]
    wide, pair, tall = rest[len(steps) + outputs :]
    load_pair(steps, xs, wide, pair)
    picked = jnp.dot(select_ref[...], pair[...], preferred_element_type=jnp.float32)
    store_rows(picked, tall, outs)


def twin_kernel(steps, select_ref, *rest):
    count = len(steps)
    own, other = rest[:count], rest[count : 2 * count]
    outs = rest[2 * count : 2 * count + 4]
    wide, pair, tall = rest[2 * count + 4 :]
    odd = lax.axis_index("chan") & 1
    rows = select_ref.shape[0] // 2
    load_pair(steps, own, wide.at[0], pair.at[0])
    picked = jnp.dot(select_ref[:rows], pair[0], preferred_element_type=jnp.float32)
    store_rows(picked, tall.at[0], outs[:2])
    load_pair(steps, other, wide.at[1], pair.at[1])
    top = pl.multiple_of(odd * rows, rows)
    picked = jnp.dot(select_ref[pl.ds(top, rows)], pair[1 - odd], preferred_element_type=jnp.float32)
    store_rows(picked, tall.at[1], outs[2:])


def twin(select, own, other, steps, per, slots):
    _, samples = own[0].shape
    rows, antennas = select.shape
    return pl.pallas_call(
        functools.partial(twin_kernel, steps),
        out_shape=[jax.ShapeDtypeStruct((per, slots, samples), jnp.bfloat16)] * 4,
        in_specs=[VMEM] * (1 + 2 * len(own)),
        out_specs=[VMEM] * 4,
        scratch_shapes=[
            pltpu.VMEM((2, 2 * antennas, samples), jnp.float32),
            pltpu.VMEM((2, antennas, 2 * samples), jnp.bfloat16),
            pltpu.VMEM((2, rows, samples), jnp.float32),
        ],
        compiler_params=PARAMS,
        cost_estimate=pl.CostEstimate(
            flops=2 * rows * antennas * 2 * samples, bytes_accessed=4_000_000, transcendentals=0
        ),
    )(select, *own, *other)


def gather(select, xs, steps, groups, per, slots):
    _, samples = xs[0].shape
    rows, antennas = select.shape
    return pl.pallas_call(
        functools.partial(gather_kernel, steps, groups),
        out_shape=[jax.ShapeDtypeStruct((per, slots, samples), jnp.bfloat16)] * groups,
        in_specs=[VMEM] * (1 + len(xs)),
        out_specs=[VMEM] * groups,
        scratch_shapes=[
            pltpu.VMEM((2 * antennas, samples), jnp.float32),
            pltpu.VMEM((antennas, 2 * samples), jnp.bfloat16),
            pltpu.VMEM((2 * rows, samples), jnp.float32),
        ],
        compiler_params=PARAMS,
        cost_estimate=pl.CostEstimate(
            flops=2 * rows * antennas * 2 * samples, bytes_accessed=4_000_000, transcendentals=0
        ),
    )(select, *xs)


def products(real, imag, part):
    right = jnp.concatenate([real, imag], axis=1)
    left = right if part == 0 else jnp.concatenate([imag, -real], axis=1)
    return lax.dot_general(left, right, (((1,), (1,)), ((), ())), preferred_element_type=jnp.float32)


def early_kernel(*refs):
    *parts, out = refs
    count = len(parts) // 2
    for s in range(parts[0].shape[0]):
        for part in range(2):
            total = None
            for e in range(count):
                term = products(parts[e][s], parts[count + e][s], part)
                total = term if total is None else total + term
            out[s, part] = total


def late_kernel(real, *rest):
    *imags, so_far, out, stage, sem = rest
    slots, samples = real.shape[1:]
    odd = lax.axis_index("chan") & 1
    copies = []
    for s in range(real.shape[0]):
        imag = imags[0][s]
        if len(imags) == 2:
            imag = jnp.where(jnp.full((slots, samples), odd) == 1, imags[1][s].astype(jnp.float32), imag.astype(jnp.float32))
            imag = imag.astype(jnp.bfloat16)
        for part in range(2):
            stage[s, part] = so_far[s, part] + products(real[s], imag, part)
            copy = pltpu.make_async_copy(stage.at[s, part], out.at[s, 0, part], sem.at[s, part])
            copy.start()
            copies.append(copy)
    for copy in copies:
        copy.wait()


def gram(real, imag, last):
    per, slots, samples = real[0].shape
    early = [e for e in range(len(real)) if e != last]
    ends = imag[last] if isinstance(imag[last], tuple) else (imag[last],)
    flops = 2 * per * 2 * slots * slots * 2 * samples
    so_far = pl.pallas_call(
        early_kernel,
        out_shape=jax.ShapeDtypeStruct((per, 2, slots, slots), jnp.float32),
        in_specs=[VMEM] * (2 * len(early)),
        out_specs=VMEM,
        compiler_params=PARAMS,
        cost_estimate=pl.CostEstimate(flops=flops * len(early), bytes_accessed=3_000_000, transcendentals=0),
    )(*[real[e] for e in early], *[imag[e] for e in early])
    return pl.pallas_call(
        late_kernel,
        out_shape=jax.ShapeDtypeStruct((per, 1, 2, slots, slots), jnp.float32),
        in_specs=[VMEM] * (2 + len(ends)),
        out_specs=pl.BlockSpec(memory_space=pl.ANY),
        scratch_shapes=[
            pltpu.VMEM((per, 2, slots, slots), jnp.float32),
            pltpu.SemaphoreType.DMA((per, 2)),
        ],
        compiler_params=PARAMS,
        cost_estimate=pl.CostEstimate(flops=flops, bytes_accessed=3_000_000, transcendentals=0),
    )(real[last], *ends, so_far)


def exchange(chunks, order, groups):
    got = list(chunks)
    for step in order:
        pairs = [(j, partner(j, step, groups)) for j in range(groups)]
        got[step] = lax.ppermute(chunks[step], "tm", pairs)
    return got


def across(x):
    x = lax.all_to_all(x, "chan", split_axis=0, concat_axis=1, tiled=True)
    return x.reshape(x.shape[1], x.shape[2])


CHIP_ORDER = (3, 1, 2)


def cross(chunks, chans, starts):
    got = list(chunks)
    for step in CHIP_ORDER:
        if 2 * step < chans:
            got[step] = lax.ppermute(chunks[step], "chan", [(i, i ^ (2 * step)) for i in starts])
    return got


def paired(chans, groups):
    return groups == 4 and chans in (2, 4, 8)


def steps_of(voltages, assignment, slot_subarray_index):
    groups = lax.axis_size("tm")
    chans = lax.axis_size("chan")
    subarrays = slot_subarray_index.shape[0]
    per = subarrays // groups
    order = sorted(range(1, groups), reverse=True)
    last = 2 if groups == 4 else order[0]
    first = [step for step in order if step != last]
    if not paired(chans, groups):
        select = plan(assignment, slot_subarray_index, groups, SLOT // 2)
        real = across(voltages[0])
        real = exchange(gather(select, [real], (0,), groups, per, SLOT), order, groups)
        imag = across(voltages[1])
        imag = exchange(gather(select, [imag], (0,), groups, per, SLOT), first + [last], groups)
        return gram(real, imag, last)

    steps = tuple(range(chans // 2))
    device = [(i, j, i * groups + j) for i in range(chans) for j in range(groups)]
    given = lax.ppermute(give(voltages), "chan", [(i, i ^ 1) for i in range(chans)])
    raw, reals, imags = merge(voltages, given)
    pairs = [(n, i * groups + (j ^ 2)) for i, j, n in device if i % 2 == 0]
    raw = lax.ppermute(raw, ("chan", "tm"), pairs)
    reals = cross(reals, chans, range(chans))
    select = plan(assignment, slot_subarray_index, groups, SLOT // 2)
    real = exchange(gather(select, reals, steps, groups, per, SLOT), order, groups)

    imags = cross(imags, chans, range(chans))
    far = cross(unstack(raw), chans, range(0, chans, 2))
    mine, near, third, fourth = twin(select, imags, far, steps, per, SLOT)
    pairs = [(n, i * groups + (j ^ (3 if i % 2 else 1))) for i, j, n in device]
    fourth = lax.ppermute(fourth, ("chan", "tm"), pairs)
    pairs = [(n, i * groups + (j ^ 2)) for i, j, n in device if i % 2]
    there = lax.ppermute(third, ("chan", "tm"), pairs)
    near = lax.ppermute(near, "tm", [(j, j ^ 1) for j in range(groups)])
    return gram(real, [mine, near, (third, there), fourth], last)


def solution(mesh):
    placed = (P(None, None, "chan", "tm"), P(), P())
    return jax.shard_map(
        steps_of,
        mesh=mesh,
        in_specs=placed,
        out_specs=P("tm", "chan", None, None, None),
        check_vma=False,
    )
```

```python
import functools

import jax
import jax.numpy as jnp
from jax import lax
from jax.experimental import pallas as pl
from jax.experimental.pallas import tpu as pltpu
from jax.sharding import PartitionSpec as P


SLOT = 384
LANES = 128


VMEM = pl.BlockSpec(memory_space=pltpu.VMEM)
SMEM = pl.BlockSpec(memory_space=pltpu.SMEM)
PARAMS = pltpu.CompilerParams(vmem_limit_bytes=20 * 1024 * 1024)


def partner(index, step, count):
    if count & (count - 1):
        return lax.rem(index + step, count) if not isinstance(index, int) else (index + step) % count
    return index ^ step


def relative(owner, me, count):
    if count & (count - 1):
        return lax.rem(owner - me + count, count)
    return owner ^ me


def plan_kernel(groups, half, slot_ref, owner_ref, select_ref):
    subarrays = slot_ref.shape[0]
    blocks = owner_ref.shape[0]
    per = subarrays // groups
    me = lax.axis_index("tm")
    shape = (subarrays, LANES)
    place = lax.broadcasted_iota(jnp.int32, shape, 0)
    name = jnp.zeros(shape, jnp.int32)
    for s in range(subarrays):
        name = jnp.where(place == s, slot_ref[s], name)
    base = jnp.zeros(shape, jnp.int32)
    for s in range(subarrays):
        chunk = relative(jnp.int32(s // per), me, groups) * per + s % per
        base = jnp.where(place == s, chunk * half, base)
    base = base.astype(jnp.float32)
    earlier = lax.broadcasted_iota(jnp.int32, (LANES, LANES), 0)
    later = lax.broadcasted_iota(jnp.int32, (LANES, LANES), 1)
    before = jnp.where(earlier < later, 1.0, 0.0).astype(jnp.bfloat16)
    held = [jnp.where(owner_ref[b : b + 1, :] == name, 1.0, 0.0) for b in range(blocks)]
    within = jnp.dot(
        jnp.concatenate(held, axis=0).astype(jnp.bfloat16), before, preferred_element_type=jnp.float32
    )
    run = base
    height = 256
    row = lax.broadcasted_iota(jnp.int32, (height, LANES), 0).astype(jnp.float32)
    for b in range(blocks):
        rank = within[b * subarrays : (b + 1) * subarrays] + run
        target = jnp.sum(held[b] * rank, axis=0, keepdims=True)
        run = run + jnp.sum(held[b], axis=1, keepdims=True)
        for top in range(0, select_ref.shape[0], height):
            hit = row == (target - top)
            select_ref[top : top + height, b * LANES : (b + 1) * LANES] = jnp.where(hit, 1.0, 0.0).astype(
                jnp.bfloat16
            )


def plan(assignment, slot_subarray_index, groups, half):
    antennas = assignment.shape[0]
    subarrays = slot_subarray_index.shape[0]
    return pl.pallas_call(
        functools.partial(plan_kernel, groups, half),
        out_shape=jax.ShapeDtypeStruct((subarrays * half, antennas), jnp.bfloat16),
        in_specs=[SMEM, VMEM],
        out_specs=VMEM,
        compiler_params=PARAMS,
        cost_estimate=pl.CostEstimate(flops=4_000_000_000, bytes_accessed=3_000_000, transcendentals=0),
    )(slot_subarray_index, assignment.reshape(antennas // LANES, LANES))


def give_kernel(chips, x_ref, out):
    me = lax.axis_index("chan")
    for k in range(2):
        for t in range(chips):
            out[k, t] = x_ref[k, (me ^ (2 * t)) ^ 1]


def give(voltages):
    parts, chans, inputs, samples = voltages.shape
    return pl.pallas_call(
        functools.partial(give_kernel, chans // 2),
        out_shape=jax.ShapeDtypeStruct((parts, chans // 2, inputs, samples), voltages.dtype),
        in_specs=[VMEM],
        out_specs=VMEM,
        compiler_params=PARAMS,
        cost_estimate=pl.CostEstimate(flops=1_000_000, bytes_accessed=1_000_000, transcendentals=0),
    )(voltages)


def merge_kernel(chips, x_ref, given_ref, *outs):
    me = lax.axis_index("chan")
    inputs = x_ref.shape[2]
    mine = pl.multiple_of((me & 1) * inputs, inputs)
    theirs = pl.multiple_of(inputs - (me & 1) * inputs, inputs)
    for k in range(2):
        for t in range(chips):
            out = outs[k * chips + t]
            piece, other = x_ref[k, me ^ (2 * t)], given_ref[k, t]
            out[pl.ds(mine, inputs)] = piece
            out[pl.ds(theirs, inputs)] = other


def merge(voltages, given):
    parts, chans, inputs, samples = voltages.shape
    chips = chans // 2
    piece = jax.ShapeDtypeStruct((2 * inputs, samples), voltages.dtype)
    out = pl.pallas_call(
        functools.partial(merge_kernel, chips),
        out_shape=[piece] * (parts * chips),
        in_specs=[VMEM] * 2,
        out_specs=[VMEM] * (parts * chips),
        compiler_params=PARAMS,
        cost_estimate=pl.CostEstimate(flops=1_000_000, bytes_accessed=2_000_000, transcendentals=0),
    )(voltages, given)
    return out[:chips], out[chips:]


def load_pair(steps, xs, wide, pair):
    inputs = xs[0].shape[0]
    antennas = inputs // 2
    chip = lax.axis_index("chan") // 2
    for i, (step, x) in enumerate(zip(steps, xs)):
        wide[i * inputs : (i + 1) * inputs] = x[...].astype(jnp.float32)
        if len(steps) == 1:
            top = 0
        else:
            top = pl.multiple_of((chip ^ step) * antennas, antennas)
        for pol in range(2):
            pair[pl.ds(top, antennas), pol * LANES : (pol + 1) * LANES] = wide[
                pl.ds(i * inputs + pol, antennas, stride=2), :
            ].astype(jnp.bfloat16)


def store_rows(picked, tall, outs):
    rows = picked.shape[0]
    for pol in range(2):
        tall[pl.ds(pol, rows, stride=2), :] = picked[:, pol * LANES : (pol + 1) * LANES]
    per, slots, _ = outs[0].shape
    for g, out in enumerate(outs):
        for s in range(per):
            top = (g * per + s) * slots
            out[s] = tall[top : top + slots, :].astype(jnp.bfloat16)


def gather_kernel(steps, outputs, select_ref, *rest):
    xs, outs = rest[: len(steps)], rest[len(steps) : len(steps) + outputs]
    wide, pair, tall = rest[len(steps) + outputs :]
    load_pair(steps, xs, wide, pair)
    picked = jnp.dot(select_ref[...], pair[...], preferred_element_type=jnp.float32)
    store_rows(picked, tall, outs)


def gather(select, xs, steps, groups, per, slots):
    _, samples = xs[0].shape
    rows, antennas = select.shape
    return pl.pallas_call(
        functools.partial(gather_kernel, steps, groups),
        out_shape=[jax.ShapeDtypeStruct((per, slots, samples), jnp.bfloat16)] * groups,
        in_specs=[VMEM] * (1 + len(xs)),
        out_specs=[VMEM] * groups,
        scratch_shapes=[
            pltpu.VMEM((2 * antennas, samples), jnp.float32),
            pltpu.VMEM((antennas, 2 * samples), jnp.bfloat16),
            pltpu.VMEM((2 * rows, samples), jnp.float32),
        ],
        compiler_params=PARAMS,
        cost_estimate=pl.CostEstimate(
            flops=2 * rows * antennas * 2 * samples, bytes_accessed=4_000_000, transcendentals=0
        ),
    )(select, *xs)


def products(real, imag, part):
    right = jnp.concatenate([real, imag], axis=1)
    left = right if part == 0 else jnp.concatenate([imag, -real], axis=1)
    return lax.dot_general(left, right, (((1,), (1,)), ((), ())), preferred_element_type=jnp.float32)


def early_kernel(*refs):
    *parts, out = refs
    count = len(parts) // 2
    for s in range(parts[0].shape[0]):
        for part in range(2):
            total = None
            for e in range(count):
                term = products(parts[e][s], parts[count + e][s], part)
                total = term if total is None else total + term
            out[s, part] = total


def late_kernel(real, imag, so_far, out, stage, sem):
    copies = []
    for s in range(real.shape[0]):
        for part in range(2):
            stage[s, part] = so_far[s, part] + products(real[s], imag[s], part)
            copy = pltpu.make_async_copy(stage.at[s, part], out.at[s, 0, part], sem.at[s, part])
            copy.start()
            copies.append(copy)
    for copy in copies:
        copy.wait()


def gram(real, imag, last):
    per, slots, samples = real[0].shape
    early = [e for e in range(len(real)) if e != last]
    flops = 2 * per * 2 * slots * slots * 2 * samples
    so_far = pl.pallas_call(
        early_kernel,
        out_shape=jax.ShapeDtypeStruct((per, 2, slots, slots), jnp.float32),
        in_specs=[VMEM] * (2 * len(early)),
        out_specs=VMEM,
        compiler_params=PARAMS,
        cost_estimate=pl.CostEstimate(flops=flops * len(early), bytes_accessed=3_000_000, transcendentals=0),
    )(*[real[e] for e in early], *[imag[e] for e in early])
    return pl.pallas_call(
        late_kernel,
        out_shape=jax.ShapeDtypeStruct((per, 1, 2, slots, slots), jnp.float32),
        in_specs=[VMEM] * 3,
        out_specs=pl.BlockSpec(memory_space=pl.ANY),
        scratch_shapes=[
            pltpu.VMEM((per, 2, slots, slots), jnp.float32),
            pltpu.SemaphoreType.DMA((per, 2)),
        ],
        compiler_params=PARAMS,
        cost_estimate=pl.CostEstimate(flops=flops, bytes_accessed=3_000_000, transcendentals=0),
    )(real[last], imag[last], so_far)


def exchange(chunks, order, groups):
    got = list(chunks)
    for step in order:
        pairs = [(j, partner(j, step, groups)) for j in range(groups)]
        got[step] = lax.ppermute(chunks[step], "tm", pairs)
    return got


def across(x):
    x = lax.all_to_all(x, "chan", split_axis=0, concat_axis=1, tiled=True)
    return x.reshape(x.shape[1], x.shape[2])


CHIP_ORDER = (3, 1, 2)


def cross(chunks, chans, starts):
    got = list(chunks)
    for step in CHIP_ORDER:
        if 2 * step < chans:
            got[step] = lax.ppermute(chunks[step], "chan", [(i, i ^ (2 * step)) for i in starts])
    return got


def by_chip(chans):
    return chans in (2, 4, 8)


def orders(groups):
    last = 2 if groups == 4 else groups - 1
    rest = [step for step in range(groups - 1, 0, -1) if step != last]
    return rest[:1] + [last] + rest[1:], rest + [last], last


def steps_of(voltages, assignment, slot_subarray_index):
    groups = lax.axis_size("tm")
    chans = lax.axis_size("chan")
    subarrays = slot_subarray_index.shape[0]
    per = subarrays // groups
    first, second, last = orders(groups)
    if by_chip(chans):
        steps = tuple(range(chans // 2))
        given = lax.ppermute(give(voltages), "chan", [(i, i ^ 1) for i in range(chans)])
        reals, imags = merge(voltages, given)
        reals = cross(reals, chans, range(chans))
        imags = cross(imags, chans, range(chans))
    else:
        steps = (0,)
        reals = [across(voltages[0])]
        imags = [across(voltages[1])]
    select = plan(assignment, slot_subarray_index, groups, SLOT // 2)
    real = exchange(gather(select, reals, steps, groups, per, SLOT), first, groups)
    imag = exchange(gather(select, imags, steps, groups, per, SLOT), second, groups)
    return gram(real, imag, last)


def solution(mesh):
    placed = (P(None, None, "chan", "tm"), P(), P())
    return jax.shard_map(
        steps_of,
        mesh=mesh,
        in_specs=placed,
        out_specs=P("tm", "chan", None, None, None),
        check_vma=False,
    )
```

```python
import functools

import jax
import jax.numpy as jnp
from jax import lax
from jax.experimental import pallas as pl
from jax.experimental.pallas import tpu as pltpu
from jax.sharding import PartitionSpec as P


SLOT = 384
LANES = 128


VMEM = pl.BlockSpec(memory_space=pltpu.VMEM)
SMEM = pl.BlockSpec(memory_space=pltpu.SMEM)
PARAMS = pltpu.CompilerParams(vmem_limit_bytes=20 * 1024 * 1024)


def partner(index, step, count):
    if count & (count - 1):
        return lax.rem(index + step, count) if not isinstance(index, int) else (index + step) % count
    return index ^ step


def relative(owner, me, count):
    if count & (count - 1):
        return lax.rem(owner - me + count, count)
    return owner ^ me


GRAIN = 32


def sizes(inputs, subarrays, groups):
    total = subarrays // groups * SLOT
    base = min(total, -(-inputs // (groups * GRAIN)) * GRAIN)
    return total, base, list(range(GRAIN, total - base + 1, GRAIN))


def plan_kernel(groups, base_rows, slot_ref, owner_ref, select_ref, place_ref, class_ref):
    subarrays = slot_ref.shape[0]
    blocks = owner_ref.shape[0]
    per = subarrays // groups
    half = SLOT // 2
    me = lax.axis_index("tm")
    shape = (subarrays, LANES)
    place = lax.broadcasted_iota(jnp.int32, shape, 0)
    name = jnp.zeros(shape, jnp.int32)
    for s in range(subarrays):
        name = jnp.where(place == s, slot_ref[s], name)
    held = [jnp.where(owner_ref[b : b + 1, :] == name, 1.0, 0.0) for b in range(blocks)]
    counts = [jnp.sum(one, axis=1, keepdims=True) for one in held]
    count = jnp.broadcast_to(sum(counts), shape)
    ahead = jnp.zeros(shape, jnp.float32)
    full = jnp.zeros(shape, jnp.float32)
    for s in range(subarrays):
        mates = jnp.logical_and(place >= s // per * per, place < (s // per + 1) * per)
        row = jnp.broadcast_to(count[s : s + 1, :], shape)
        full = full + jnp.where(mates, row, 0.0)
        ahead = ahead + jnp.where(jnp.logical_and(mates, place > s), row, 0.0)
    rest = 2 * jnp.max(full).astype(jnp.int32) - base_rows
    class_ref[0] = jnp.maximum((rest + GRAIN - 1) // GRAIN - 1, 0)

    start = jnp.zeros(shape, jnp.float32)
    for s in range(subarrays):
        chunk = relative(jnp.int32(s // per), me, groups)
        top = (chunk * (per * half)).astype(jnp.float32)
        mine = jnp.where(chunk == 0, 1.0, 0.0)
        inside = mine * (s % per * half) + (1.0 - mine) * ahead
        start = jnp.where(place == s, top + inside, start)
    earlier = lax.broadcasted_iota(jnp.int32, (LANES, LANES), 0)
    later = lax.broadcasted_iota(jnp.int32, (LANES, LANES), 1)
    before = jnp.where(earlier < later, 1.0, 0.0).astype(jnp.bfloat16)
    within = jnp.dot(
        jnp.concatenate(held, axis=0).astype(jnp.bfloat16), before, preferred_element_type=jnp.float32
    )
    run = start
    height = 256
    row = lax.broadcasted_iota(jnp.int32, (height, LANES), 0).astype(jnp.float32)
    for b in range(blocks):
        rank = within[b * subarrays : (b + 1) * subarrays] + run
        target = jnp.sum(held[b] * rank, axis=0, keepdims=True)
        run = run + counts[b]
        for top in range(0, select_ref.shape[0], height):
            hit = row == (target - top)
            select_ref[top : top + height, b * LANES : (b + 1) * LANES] = jnp.where(hit, 1.0, 0.0).astype(
                jnp.bfloat16
            )
    rank = lax.broadcasted_iota(jnp.int32, (SLOT, LANES), 0).astype(jnp.float32)
    column = lax.broadcasted_iota(jnp.int32, (SLOT, LANES), 1).astype(jnp.float32)
    for s in range(per):
        own = place == me * per + s
        held_here = 2 * jnp.sum(jnp.where(own, count, 0.0), axis=0, keepdims=True)
        offset = 2 * jnp.sum(jnp.where(own, ahead, 0.0), axis=0, keepdims=True)
        target = jnp.where(rank < held_here, rank + offset, -1.0)
        for left in range(0, place_ref.shape[1], LANES):
            place_ref[s * SLOT : (s + 1) * SLOT, left : left + LANES] = jnp.where(
                column == target - left, 1.0, 0.0
            ).astype(jnp.bfloat16)


def plan(assignment, slot_subarray_index, groups, base):
    antennas = assignment.shape[0]
    subarrays = slot_subarray_index.shape[0]
    total = subarrays // groups * SLOT
    return pl.pallas_call(
        functools.partial(plan_kernel, groups, base),
        out_shape=[
            jax.ShapeDtypeStruct((subarrays * SLOT // 2, antennas), jnp.bfloat16),
            jax.ShapeDtypeStruct((total, total), jnp.bfloat16),
            jax.ShapeDtypeStruct((1,), jnp.int32),
        ],
        in_specs=[SMEM, VMEM],
        out_specs=[VMEM, VMEM, SMEM],
        compiler_params=PARAMS,
        cost_estimate=pl.CostEstimate(flops=4_000_000_000, bytes_accessed=4_000_000, transcendentals=0),
    )(slot_subarray_index, assignment.reshape(antennas // LANES, LANES))


def give_kernel(chips, x_ref, out):
    me = lax.axis_index("chan")
    for k in range(2):
        for t in range(chips):
            out[k, t] = x_ref[k, (me ^ (2 * t)) ^ 1]


def give(voltages):
    parts, chans, inputs, samples = voltages.shape
    return pl.pallas_call(
        functools.partial(give_kernel, chans // 2),
        out_shape=jax.ShapeDtypeStruct((parts, chans // 2, inputs, samples), voltages.dtype),
        in_specs=[VMEM],
        out_specs=VMEM,
        compiler_params=PARAMS,
        cost_estimate=pl.CostEstimate(flops=1_000_000, bytes_accessed=1_000_000, transcendentals=0),
    )(voltages)


def merge_kernel(chips, x_ref, given_ref, *outs):
    me = lax.axis_index("chan")
    inputs = x_ref.shape[2]
    mine = pl.multiple_of((me & 1) * inputs, inputs)
    theirs = pl.multiple_of(inputs - (me & 1) * inputs, inputs)
    for k in range(2):
        for t in range(chips):
            out = outs[k * chips + t]
            piece, other = x_ref[k, me ^ (2 * t)], given_ref[k, t]
            out[pl.ds(mine, inputs)] = piece
            out[pl.ds(theirs, inputs)] = other


def merge(voltages, given):
    parts, chans, inputs, samples = voltages.shape
    chips = chans // 2
    piece = jax.ShapeDtypeStruct((2 * inputs, samples), voltages.dtype)
    out = pl.pallas_call(
        functools.partial(merge_kernel, chips),
        out_shape=[piece] * (parts * chips),
        in_specs=[VMEM] * 2,
        out_specs=[VMEM] * (parts * chips),
        compiler_params=PARAMS,
        cost_estimate=pl.CostEstimate(flops=1_000_000, bytes_accessed=2_000_000, transcendentals=0),
    )(voltages, given)
    return out[:chips], out[chips:]


def load_pair(steps, xs, wide, pair):
    inputs = xs[0].shape[0]
    antennas = inputs // 2
    chip = lax.axis_index("chan") // 2
    for i, (step, x) in enumerate(zip(steps, xs)):
        wide[i * inputs : (i + 1) * inputs] = x[...].astype(jnp.float32)
        if len(steps) == 1:
            top = 0
        else:
            top = pl.multiple_of((chip ^ step) * antennas, antennas)
        for pol in range(2):
            pair[pl.ds(top, antennas), pol * LANES : (pol + 1) * LANES] = wide[
                pl.ds(i * inputs + pol, antennas, stride=2), :
            ].astype(jnp.bfloat16)


def gather_kernel(steps, groups, after, select_ref, *rest):
    xs, rest = rest[: len(steps)], rest[len(steps) :]
    if after:
        reals, rest = rest[: groups - 1], rest[groups - 1 :]
    own, bases, rests = rest[0], rest[1:groups], rest[groups : 2 * groups - 1]
    wide, pair, tall = rest[2 * groups - 1 :]
    load_pair(steps, xs, wide, pair)
    picked = jnp.dot(select_ref[...], pair[...], preferred_element_type=jnp.float32)
    rows = picked.shape[0]
    for pol in range(2):
        tall[pl.ds(pol, rows, stride=2), :] = picked[:, pol * LANES : (pol + 1) * LANES]
    per, slots, _ = own.shape
    for s in range(per):
        own[s] = tall[s * slots : (s + 1) * slots, :].astype(jnp.bfloat16)
    for i in range(groups - 1):
        top = (i + 1) * per * slots
        middle = top + bases[i].shape[0]
        bases[i][...] = tall[top:middle, :].astype(jnp.bfloat16)
        end = top + per * slots
        if after:
            rests[i][:, :LANES] = reals[i][...]
            rests[i][:, LANES:] = tall[middle:end, :].astype(jnp.bfloat16)
        else:
            rests[i][...] = tall[middle:end, :].astype(jnp.bfloat16)


def gather(select, xs, steps, groups, per, base, reals=()):
    _, samples = xs[0].shape
    rows, antennas = select.shape
    rest = per * SLOT - base
    out = pl.pallas_call(
        functools.partial(gather_kernel, steps, groups, bool(reals)),
        out_shape=[jax.ShapeDtypeStruct((per, SLOT, samples), jnp.bfloat16)]
        + [jax.ShapeDtypeStruct((base, samples), jnp.bfloat16)] * (groups - 1)
        + [jax.ShapeDtypeStruct((rest, (2 if reals else 1) * samples), jnp.bfloat16)] * (groups - 1),
        in_specs=[VMEM] * (1 + len(xs) + len(reals)),
        out_specs=[VMEM] * (2 * groups - 1),
        scratch_shapes=[
            pltpu.VMEM((2 * antennas, samples), jnp.float32),
            pltpu.VMEM((antennas, 2 * samples), jnp.bfloat16),
            pltpu.VMEM((2 * rows, samples), jnp.float32),
        ],
        compiler_params=PARAMS,
        cost_estimate=pl.CostEstimate(
            flops=2 * rows * antennas * 2 * samples, bytes_accessed=4_000_000, transcendentals=0
        ),
    )(select, *xs, *reals)
    return out[0], [None] + list(out[1:groups]), list(out[groups:])


def products(both, part):
    samples = both.shape[1] // 2
    left = both
    if part:
        left = jnp.concatenate([both[:, samples:], -both[:, :samples]], axis=1)
    return lax.dot_general(left, both, (((1,), (1,)), ((), ())), preferred_element_type=jnp.float32)


def unpack(place_ref, real, imag, rest, packed):
    base, samples = real.shape
    packed[:base, :samples] = real[...]
    packed[:base, samples:] = imag[...]
    packed[base:, :] = rest[...]
    return jnp.dot(place_ref[...], packed[...], preferred_element_type=jnp.float32).astype(jnp.bfloat16)


def early_kernel(place_ref, own_real, own_imag, *refs):
    *parts, out, packed = refs
    count = len(parts) // 3
    blocks = [unpack(place_ref, *parts[3 * e : 3 * e + 3], packed.at[e]) for e in range(count)]
    for s in range(own_real.shape[0]):
        both = [jnp.concatenate([own_real[s], own_imag[s]], axis=1)]
        both += [block[s * SLOT : (s + 1) * SLOT] for block in blocks]
        for part in range(2):
            out[s, part] = sum(products(one, part) for one in both)


def late_kernel(place_ref, real, imag, rest, so_far, out, packed, stage, sem):
    block = unpack(place_ref, real, imag, rest, packed)
    copies = []
    for s in range(out.shape[0]):
        for part in range(2):
            stage[s, part] = so_far[s, part] + products(block[s * SLOT : (s + 1) * SLOT], part)
            copy = pltpu.make_async_copy(stage.at[s, part], out.at[s, 0, part], sem.at[s, part])
            copy.start()
            copies.append(copy)
    for copy in copies:
        copy.wait()


def gram(place, own, real, imag, rest, last):
    per, slots, samples = own[0].shape
    total = per * slots
    early = [e for e in range(1, len(real)) if e != last]
    flops = 2 * per * 2 * slots * slots * 2 * samples
    so_far = pl.pallas_call(
        early_kernel,
        out_shape=jax.ShapeDtypeStruct((per, 2, slots, slots), jnp.float32),
        in_specs=[VMEM] * (3 + 3 * len(early)),
        out_specs=VMEM,
        scratch_shapes=[pltpu.VMEM((len(early), total, 2 * samples), jnp.bfloat16)],
        compiler_params=PARAMS,
        cost_estimate=pl.CostEstimate(flops=flops * len(real), bytes_accessed=3_000_000, transcendentals=0),
    )(place, *own, *[x for e in early for x in (real[e], imag[e], rest[e - 1])])
    return pl.pallas_call(
        late_kernel,
        out_shape=jax.ShapeDtypeStruct((per, 1, 2, slots, slots), jnp.float32),
        in_specs=[VMEM] * 5,
        out_specs=pl.BlockSpec(memory_space=pl.ANY),
        scratch_shapes=[
            pltpu.VMEM((total, 2 * samples), jnp.bfloat16),
            pltpu.VMEM((per, 2, slots, slots), jnp.float32),
            pltpu.SemaphoreType.DMA((per, 2)),
        ],
        compiler_params=PARAMS,
        cost_estimate=pl.CostEstimate(flops=flops, bytes_accessed=3_000_000, transcendentals=0),
    )(place, real[last], imag[last], rest[last - 1], so_far)


def hop(x, step, groups):
    return lax.ppermute(x, "tm", [(j, partner(j, step, groups)) for j in range(groups)])


def exchange(chunks, order, groups):
    got = list(chunks)
    for step in order:
        got[step] = hop(chunks[step], step, groups)
    return got


def exchange_rest(chunks, size_class, rows, groups):
    def send(count):
        def branch(*chunks):
            got = [hop(x[:count], i + 1, groups) for i, x in enumerate(chunks)]
            return [jnp.pad(x, ((0, chunks[0].shape[0] - count), (0, 0))) for x in got]

        return branch

    return lax.switch(size_class, [send(count) for count in rows], *chunks)


def across(x):
    x = lax.all_to_all(x, "chan", split_axis=0, concat_axis=1, tiled=True)
    return x.reshape(x.shape[1], x.shape[2])


CHIP_ORDER = (3, 1, 2)


def cross(chunks, chans, starts):
    got = list(chunks)
    for step in CHIP_ORDER:
        if 2 * step < chans:
            got[step] = lax.ppermute(chunks[step], "chan", [(i, i ^ (2 * step)) for i in starts])
    return got


def by_chip(chans):
    return chans in (2, 4, 8)


def orders(groups):
    last = 2 if groups == 4 else groups - 1
    rest = [step for step in range(groups - 1, 0, -1) if step != last]
    return rest[:1] + [last] + rest[1:], rest + [last], last


def steps_of(voltages, assignment, slot_subarray_index):
    groups = lax.axis_size("tm")
    chans = lax.axis_size("chan")
    subarrays = slot_subarray_index.shape[0]
    per = subarrays // groups
    first, second, last = orders(groups)
    if by_chip(chans):
        steps = tuple(range(chans // 2))
        given = lax.ppermute(give(voltages), "chan", [(i, i ^ 1) for i in range(chans)])
        reals, imags = merge(voltages, given)
        reals = cross(reals, chans, range(chans))
        imags = cross(imags, chans, range(chans))
    else:
        steps = (0,)
        reals = [across(voltages[0])]
        imags = [across(voltages[1])]
    _, base, rows = sizes(2 * assignment.shape[0], subarrays, groups)
    select, place, size_class = plan(assignment, slot_subarray_index, groups, base)
    own_real, real, real_rest = gather(select, reals, steps, groups, per, base)
    real = exchange(real, first, groups)
    own_imag, imag, rest = gather(select, imags, steps, groups, per, base, real_rest)
    imag = exchange(imag, second, groups)
    rest = exchange_rest(rest, size_class[0], rows, groups)
    return gram(place, (own_real, own_imag), real, imag, rest, last)


def solution(mesh):
    placed = (P(None, None, "chan", "tm"), P(), P())
    return jax.shard_map(
        steps_of,
        mesh=mesh,
        in_specs=placed,
        out_specs=P("tm", "chan", None, None, None),
        check_vma=False,
    )
```

```python
import functools

import jax
import jax.numpy as jnp
from jax import lax
from jax.experimental import pallas as pl
from jax.experimental.pallas import tpu as pltpu
from jax.sharding import PartitionSpec as P


SLOT = 384
LANES = 128


VMEM = pl.BlockSpec(memory_space=pltpu.VMEM)
SMEM = pl.BlockSpec(memory_space=pltpu.SMEM)
PARAMS = pltpu.CompilerParams(vmem_limit_bytes=20 * 1024 * 1024)


def partner(index, step, count):
    if count & (count - 1):
        return lax.rem(index + step, count) if not isinstance(index, int) else (index + step) % count
    return index ^ step


def relative(owner, me, count):
    if count & (count - 1):
        return lax.rem(owner - me + count, count)
    return owner ^ me


def plan_kernel(groups, half, slot_ref, owner_ref, select_ref):
    subarrays = slot_ref.shape[0]
    blocks = owner_ref.shape[0]
    per = subarrays // groups
    me = lax.axis_index("tm")
    shape = (subarrays, LANES)
    place = lax.broadcasted_iota(jnp.int32, shape, 0)
    name = jnp.zeros(shape, jnp.int32)
    for s in range(subarrays):
        name = jnp.where(place == s, slot_ref[s], name)
    base = jnp.zeros(shape, jnp.int32)
    for s in range(subarrays):
        chunk = relative(jnp.int32(s // per), me, groups) * per + s % per
        base = jnp.where(place == s, chunk * half, base)
    base = base.astype(jnp.float32)
    earlier = lax.broadcasted_iota(jnp.int32, (LANES, LANES), 0)
    later = lax.broadcasted_iota(jnp.int32, (LANES, LANES), 1)
    before = jnp.where(earlier < later, 1.0, 0.0).astype(jnp.bfloat16)
    held = [jnp.where(owner_ref[b : b + 1, :] == name, 1.0, 0.0) for b in range(blocks)]
    within = jnp.dot(
        jnp.concatenate(held, axis=0).astype(jnp.bfloat16), before, preferred_element_type=jnp.float32
    )
    run = base
    height = 256
    row = lax.broadcasted_iota(jnp.int32, (height, LANES), 0).astype(jnp.float32)
    for b in range(blocks):
        rank = within[b * subarrays : (b + 1) * subarrays] + run
        target = jnp.sum(held[b] * rank, axis=0, keepdims=True)
        run = run + jnp.sum(held[b], axis=1, keepdims=True)
        for top in range(0, select_ref.shape[0], height):
            hit = row == (target - top)
            select_ref[top : top + height, b * LANES : (b + 1) * LANES] = jnp.where(hit, 1.0, 0.0).astype(
                jnp.bfloat16
            )


def plan(assignment, slot_subarray_index, groups, half):
    antennas = assignment.shape[0]
    subarrays = slot_subarray_index.shape[0]
    return pl.pallas_call(
        functools.partial(plan_kernel, groups, half),
        out_shape=jax.ShapeDtypeStruct((subarrays * half, antennas), jnp.bfloat16),
        in_specs=[SMEM, VMEM],
        out_specs=VMEM,
        compiler_params=PARAMS,
        cost_estimate=pl.CostEstimate(flops=4_000_000_000, bytes_accessed=3_000_000, transcendentals=0),
    )(slot_subarray_index, assignment.reshape(antennas // LANES, LANES))


def give_kernel(chips, x_ref, *outs):
    me = lax.axis_index("chan")
    for k, out in enumerate(outs):
        for t in range(chips):
            out[t] = x_ref[k, (me ^ (2 * t)) ^ 1]


def give(voltages):
    parts, chans, inputs, samples = voltages.shape
    return pl.pallas_call(
        functools.partial(give_kernel, chans // 2),
        out_shape=[jax.ShapeDtypeStruct((chans // 2, inputs, samples), voltages.dtype)] * parts,
        in_specs=[VMEM],
        out_specs=[VMEM] * parts,
        compiler_params=PARAMS,
        cost_estimate=pl.CostEstimate(flops=1_000_000, bytes_accessed=1_000_000, transcendentals=0),
    )(voltages)


def fold(a, b):
    half = LANES // 2
    left = lax.broadcasted_iota(jnp.int32, a.shape, 1) < half
    return (
        jnp.where(left, a, pltpu.roll(b, half, 1)),
        jnp.where(left, pltpu.roll(a, half, 1), b),
    )


def merge_halves_kernel(chips, x_ref, given_ref, *outs):
    me = lax.axis_index("chan")
    for parity in range(2):

        @pl.when((me & 1) == parity)
        def _():
            for t in range(chips):
                cores = [x_ref[0, me ^ (2 * t)], given_ref[t]]
                if parity:
                    cores.reverse()
                for h, half in enumerate(fold(*[core.astype(jnp.float32) for core in cores])):
                    outs[h * chips + t][...] = half.astype(jnp.bfloat16)


def merge_kernel(chips, x_ref, given_ref, *outs):
    me = lax.axis_index("chan")
    inputs = x_ref.shape[2]
    mine = pl.multiple_of((me & 1) * inputs, inputs)
    theirs = pl.multiple_of(inputs - (me & 1) * inputs, inputs)
    for t in range(chips):
        outs[t][pl.ds(mine, inputs)] = x_ref[1, me ^ (2 * t)]
        outs[t][pl.ds(theirs, inputs)] = given_ref[t]


def merge(kernel, height, voltages, given):
    _, chans, inputs, samples = voltages.shape
    chips = chans // 2
    count = 2 * chips // height
    return pl.pallas_call(
        functools.partial(kernel, chips),
        out_shape=[jax.ShapeDtypeStruct((height * inputs, samples), voltages.dtype)] * count,
        in_specs=[VMEM] * 2,
        out_specs=[VMEM] * count,
        compiler_params=PARAMS,
        cost_estimate=pl.CostEstimate(flops=1_000_000, bytes_accessed=1_000_000, transcendentals=0),
    )(voltages, given)


def gather_half_kernel(steps, groups, select_ref, *rest):
    xs, outs = rest[: len(steps)], rest[len(steps) : len(steps) + groups]
    wide, pair = rest[len(steps) + groups :]
    inputs = xs[0].shape[0]
    each = inputs // 2
    chip = lax.axis_index("chan") // 2
    for i, (step, x) in enumerate(zip(steps, xs)):
        wide[i * inputs : (i + 1) * inputs] = x[...].astype(jnp.float32)
        pols = [wide[pl.ds(i * inputs + pol, each, stride=2), :] for pol in range(2)]
        top = (chip ^ step) * inputs
        for core, one in enumerate(fold(*pols)):
            pair[pl.ds(pl.multiple_of(top + core * each, each), each)] = one.astype(jnp.bfloat16)
    picked = jnp.dot(select_ref[...], pair[...], preferred_element_type=jnp.float32)
    per, rows, _ = outs[0].shape
    for g, out in enumerate(outs):
        for s in range(per):
            top = (g * per + s) * rows
            out[s] = picked[top : top + rows].astype(jnp.bfloat16)


def gather_half(select, xs, steps, groups, per):
    inputs, samples = xs[0].shape
    rows, antennas = select.shape
    return pl.pallas_call(
        functools.partial(gather_half_kernel, steps, groups),
        out_shape=[jax.ShapeDtypeStruct((per, rows // (groups * per), samples), jnp.bfloat16)] * groups,
        in_specs=[VMEM] * (1 + len(xs)),
        out_specs=[VMEM] * groups,
        scratch_shapes=[
            pltpu.VMEM((inputs * len(xs), samples), jnp.float32),
            pltpu.VMEM((antennas, samples), jnp.bfloat16),
        ],
        compiler_params=PARAMS,
        cost_estimate=pl.CostEstimate(
            flops=2 * rows * antennas * samples, bytes_accessed=4_000_000, transcendentals=0
        ),
    )(select, *xs)


def join_kernel(*refs):
    *parts, tall = refs
    count = len(parts) // 3
    for e in range(count):
        first, second, out = parts[e], parts[count + e], parts[2 * count + e]
        per, rows, _ = first.shape
        for s in range(per):
            for pol, one in enumerate(fold(first[s].astype(jnp.float32), second[s].astype(jnp.float32))):
                tall[e * per + s, pl.ds(pol, rows, stride=2), :] = one
            out[s] = tall[e * per + s].astype(jnp.bfloat16)


def join(first, second):
    per, rows, samples = first[0].shape
    count = len(first)
    return pl.pallas_call(
        join_kernel,
        out_shape=[jax.ShapeDtypeStruct((per, 2 * rows, samples), jnp.bfloat16)] * count,
        in_specs=[VMEM] * (2 * count),
        out_specs=[VMEM] * count,
        scratch_shapes=[pltpu.VMEM((count * per, 2 * rows, samples), jnp.float32)],
        compiler_params=PARAMS,
        cost_estimate=pl.CostEstimate(flops=1_000_000, bytes_accessed=2_000_000, transcendentals=0),
    )(*first, *second)


def load_pair(steps, xs, wide, pair):
    inputs = xs[0].shape[0]
    antennas = inputs // 2
    chip = lax.axis_index("chan") // 2
    for i, (step, x) in enumerate(zip(steps, xs)):
        wide[i * inputs : (i + 1) * inputs] = x[...].astype(jnp.float32)
        if len(steps) == 1:
            top = 0
        else:
            top = pl.multiple_of((chip ^ step) * antennas, antennas)
        for pol in range(2):
            pair[pl.ds(top, antennas), pol * LANES : (pol + 1) * LANES] = wide[
                pl.ds(i * inputs + pol, antennas, stride=2), :
            ].astype(jnp.bfloat16)


def store_rows(picked, tall, outs):
    rows = picked.shape[0]
    for pol in range(2):
        tall[pl.ds(pol, rows, stride=2), :] = picked[:, pol * LANES : (pol + 1) * LANES]
    per, slots, _ = outs[0].shape
    for g, out in enumerate(outs):
        for s in range(per):
            top = (g * per + s) * slots
            out[s] = tall[top : top + slots, :].astype(jnp.bfloat16)


def gather_kernel(steps, outputs, select_ref, *rest):
    xs, outs = rest[: len(steps)], rest[len(steps) : len(steps) + outputs]
    wide, pair, tall = rest[len(steps) + outputs :]
    load_pair(steps, xs, wide, pair)
    picked = jnp.dot(select_ref[...], pair[...], preferred_element_type=jnp.float32)
    store_rows(picked, tall, outs)


def gather(select, xs, steps, groups, per, slots):
    _, samples = xs[0].shape
    rows, antennas = select.shape
    return pl.pallas_call(
        functools.partial(gather_kernel, steps, groups),
        out_shape=[jax.ShapeDtypeStruct((per, slots, samples), jnp.bfloat16)] * groups,
        in_specs=[VMEM] * (1 + len(xs)),
        out_specs=[VMEM] * groups,
        scratch_shapes=[
            pltpu.VMEM((2 * antennas, samples), jnp.float32),
            pltpu.VMEM((antennas, 2 * samples), jnp.bfloat16),
            pltpu.VMEM((2 * rows, samples), jnp.float32),
        ],
        compiler_params=PARAMS,
        cost_estimate=pl.CostEstimate(
            flops=2 * rows * antennas * 2 * samples, bytes_accessed=4_000_000, transcendentals=0
        ),
    )(select, *xs)


def products(real, imag, part):
    right = jnp.concatenate([real, imag], axis=1)
    left = right if part == 0 else jnp.concatenate([imag, -real], axis=1)
    return lax.dot_general(left, right, (((1,), (1,)), ((), ())), preferred_element_type=jnp.float32)


def early_kernel(*refs):
    *parts, out = refs
    count = len(parts) // 2
    for s in range(parts[0].shape[0]):
        for part in range(2):
            total = None
            for e in range(count):
                term = products(parts[e][s], parts[count + e][s], part)
                total = term if total is None else total + term
            out[s, part] = total


def late_kernel(real, imag, so_far, out, stage, sem):
    copies = []
    for s in range(real.shape[0]):
        for part in range(2):
            stage[s, part] = so_far[s, part] + products(real[s], imag[s], part)
            copy = pltpu.make_async_copy(stage.at[s, part], out.at[s, 0, part], sem.at[s, part])
            copy.start()
            copies.append(copy)
    for copy in copies:
        copy.wait()


def gram(real, imag, last):
    per, slots, samples = real[0].shape
    early = [e for e in range(len(real)) if e != last]
    flops = 2 * per * 2 * slots * slots * 2 * samples
    so_far = pl.pallas_call(
        early_kernel,
        out_shape=jax.ShapeDtypeStruct((per, 2, slots, slots), jnp.float32),
        in_specs=[VMEM] * (2 * len(early)),
        out_specs=VMEM,
        compiler_params=PARAMS,
        cost_estimate=pl.CostEstimate(flops=flops * len(early), bytes_accessed=3_000_000, transcendentals=0),
    )(*[real[e] for e in early], *[imag[e] for e in early])
    return pl.pallas_call(
        late_kernel,
        out_shape=jax.ShapeDtypeStruct((per, 1, 2, slots, slots), jnp.float32),
        in_specs=[VMEM] * 3,
        out_specs=pl.BlockSpec(memory_space=pl.ANY),
        scratch_shapes=[
            pltpu.VMEM((per, 2, slots, slots), jnp.float32),
            pltpu.SemaphoreType.DMA((per, 2)),
        ],
        compiler_params=PARAMS,
        cost_estimate=pl.CostEstimate(flops=flops, bytes_accessed=3_000_000, transcendentals=0),
    )(real[last], imag[last], so_far)


def exchange(chunks, order, groups):
    got = list(chunks)
    for step in order:
        pairs = [(j, partner(j, step, groups)) for j in range(groups)]
        got[step] = lax.ppermute(chunks[step], "tm", pairs)
    return got


def across(x):
    x = lax.all_to_all(x, "chan", split_axis=0, concat_axis=1, tiled=True)
    return x.reshape(x.shape[1], x.shape[2])


CHIP_ORDER = (3, 1, 2)


def cross(chunks, chans, starts):
    got = list(chunks)
    for step in CHIP_ORDER:
        if 2 * step < chans:
            got[step] = lax.ppermute(chunks[step], "chan", [(i, i ^ (2 * step)) for i in starts])
    return got


def by_chip(chans):
    return chans in (2, 4, 8)


def orders(groups):
    last = 2 if groups == 4 else groups - 1
    rest = [step for step in range(groups - 1, 0, -1) if step != last]
    return rest[:1] + [last] + rest[1:], rest + [last], last


def steps_of(voltages, assignment, slot_subarray_index):
    groups = lax.axis_size("tm")
    chans = lax.axis_size("chan")
    subarrays = slot_subarray_index.shape[0]
    per = subarrays // groups
    first, second, last = orders(groups)
    if not by_chip(chans):
        steps = (0,)
        reals = [across(voltages[0])]
        imags = [across(voltages[1])]
        select = plan(assignment, slot_subarray_index, groups, SLOT // 2)
        real = exchange(gather(select, reals, steps, groups, per, SLOT), first, groups)
        imag = exchange(gather(select, imags, steps, groups, per, SLOT), second, groups)
        return gram(real, imag, last)

    chips = chans // 2
    steps = tuple(range(chips))
    swap = [(i, i ^ 1) for i in range(chans)]
    give_real, give_imag = give(voltages)
    given_real = lax.ppermute(give_real, "chan", swap)
    halves = merge(merge_halves_kernel, 1, voltages, given_real)
    given_imag = lax.ppermute(give_imag, "chan", swap)
    select = plan(assignment, slot_subarray_index, groups, SLOT // 2)
    got = []
    for h in range(2):
        pieces = cross(halves[h * chips : (h + 1) * chips], chans, range(chans))
        got.append(exchange(gather_half(select, pieces, steps, groups, per), first, groups))
    imags = cross(merge(merge_kernel, 2, voltages, given_imag), chans, range(chans))
    imag = exchange(gather(select, imags, steps, groups, per, SLOT), second, groups)
    return gram(join(*got), imag, last)


def solution(mesh):
    placed = (P(None, None, "chan", "tm"), P(), P())
    return jax.shard_map(
        steps_of,
        mesh=mesh,
        in_specs=placed,
        out_specs=P("tm", "chan", None, None, None),
        check_vma=False,
    )
```

```python
import functools

import jax
import jax.numpy as jnp
from jax import lax
from jax.experimental import pallas as pl
from jax.experimental.pallas import tpu as pltpu
from jax.sharding import PartitionSpec as P


SLOT = 384
LANES = 128


VMEM = pl.BlockSpec(memory_space=pltpu.VMEM)
PARAMS = pltpu.CompilerParams(vmem_limit_bytes=20 * 1024 * 1024)


def partner(index, step, count):
    if count & (count - 1):
        return lax.rem(index + step, count) if not isinstance(index, int) else (index + step) % count
    return index ^ step


def relative(owner, me, count):
    if count & (count - 1):
        return lax.rem(owner - me + count, count)
    return owner ^ me


def plan_kernel(groups, half, slot_ref, owner_ref, select_ref):
    subarrays = slot_ref.shape[1]
    blocks = owner_ref.shape[0]
    per = subarrays // groups
    me = lax.axis_index("tm")
    shape = (subarrays, LANES)
    place = lax.broadcasted_iota(jnp.int32, shape, 0)
    square = (subarrays, subarrays)
    diagonal = lax.broadcasted_iota(jnp.int32, square, 0) == lax.broadcasted_iota(jnp.int32, square, 1)
    slot = jnp.broadcast_to(slot_ref[...].astype(jnp.float32), square)
    name = jnp.sum(jnp.where(diagonal, slot, 0.0), axis=1, keepdims=True)
    name = jnp.broadcast_to(name, shape).astype(jnp.int32)
    base = jnp.zeros(shape, jnp.int32)
    for s in range(subarrays):
        chunk = relative(jnp.int32(s // per), me, groups) * per + s % per
        base = jnp.where(place == s, chunk * half, base)
    base = base.astype(jnp.float32)
    earlier = lax.broadcasted_iota(jnp.int32, (LANES, LANES), 0)
    later = lax.broadcasted_iota(jnp.int32, (LANES, LANES), 1)
    before = jnp.where(earlier < later, 1.0, 0.0).astype(jnp.bfloat16)
    held = [jnp.where(owner_ref[b : b + 1, :] == name, 1.0, 0.0) for b in range(blocks)]
    within = jnp.dot(
        jnp.concatenate(held, axis=0).astype(jnp.bfloat16), before, preferred_element_type=jnp.float32
    )
    run = base
    height, strip = 256, 16
    rows = lax.broadcasted_iota(jnp.int32, (strip, LANES), 0)
    strips = [(rows + top).astype(jnp.float32).astype(jnp.bfloat16) for top in range(0, height, strip)]
    one, zero = jnp.ones((strip, LANES), jnp.bfloat16), jnp.zeros((strip, LANES), jnp.bfloat16)
    for b in range(blocks):
        rank = within[b * subarrays : (b + 1) * subarrays] + run
        target = jnp.sum(held[b] * rank, axis=0, keepdims=True)
        run = run + jnp.sum(held[b], axis=1, keepdims=True)
        for top in range(0, select_ref.shape[0], height):
            inside = jnp.logical_and(target >= top, target < top + height)
            at = jnp.where(inside, target - top, -1.0)
            at = jnp.broadcast_to(at, (strip, LANES)).astype(jnp.bfloat16)
            for i, row in enumerate(strips):
                start = top + i * strip
                select_ref[start : start + strip, b * LANES : (b + 1) * LANES] = jnp.where(row == at, one, zero)


def plan(assignment, slot_subarray_index, groups, half):
    antennas = assignment.shape[0]
    subarrays = slot_subarray_index.shape[0]
    return pl.pallas_call(
        functools.partial(plan_kernel, groups, half),
        out_shape=jax.ShapeDtypeStruct((subarrays * half, antennas), jnp.bfloat16),
        in_specs=[VMEM, VMEM],
        out_specs=VMEM,
        compiler_params=PARAMS,
        cost_estimate=pl.CostEstimate(flops=4_000_000_000, bytes_accessed=3_000_000, transcendentals=0),
    )(slot_subarray_index.reshape(1, subarrays), assignment.reshape(antennas // LANES, LANES))


def give_kernel(chips, x_ref, out):
    me = lax.axis_index("chan")
    for k in range(2):
        for t in range(chips):
            out[k, t] = x_ref[k, (me ^ (2 * t)) ^ 1]


def give(voltages):
    parts, chans, inputs, samples = voltages.shape
    return pl.pallas_call(
        functools.partial(give_kernel, chans // 2),
        out_shape=jax.ShapeDtypeStruct((parts, chans // 2, inputs, samples), voltages.dtype),
        in_specs=[VMEM],
        out_specs=VMEM,
        compiler_params=PARAMS,
        cost_estimate=pl.CostEstimate(flops=1_000_000, bytes_accessed=1_000_000, transcendentals=0),
    )(voltages)


def fold(a, b):
    half = LANES // 2
    left = lax.broadcasted_iota(jnp.int32, a.shape, 1) < half
    return (
        jnp.where(left, a, pltpu.roll(b, half, 1)),
        jnp.where(left, pltpu.roll(a, half, 1), b),
    )


def merge_halves_kernel(chips, x_ref, given_ref, *outs):
    me = lax.axis_index("chan")
    for parity in range(2):

        @pl.when((me & 1) == parity)
        def _():
            for t in range(chips):
                cores = [x_ref[0, me ^ (2 * t)], given_ref[0, t]]
                if parity:
                    cores.reverse()
                for h, half in enumerate(fold(*[core.astype(jnp.float32) for core in cores])):
                    outs[h * chips + t][...] = half.astype(jnp.bfloat16)


def merge_kernel(chips, x_ref, given_ref, *outs):
    me = lax.axis_index("chan")
    inputs = x_ref.shape[2]
    mine = pl.multiple_of((me & 1) * inputs, inputs)
    theirs = pl.multiple_of(inputs - (me & 1) * inputs, inputs)
    for t in range(chips):
        outs[t][pl.ds(mine, inputs)] = x_ref[1, me ^ (2 * t)]
        outs[t][pl.ds(theirs, inputs)] = given_ref[1, t]


def merge(kernel, height, voltages, given):
    _, chans, inputs, samples = voltages.shape
    chips = chans // 2
    count = 2 * chips // height
    return pl.pallas_call(
        functools.partial(kernel, chips),
        out_shape=[jax.ShapeDtypeStruct((height * inputs, samples), voltages.dtype)] * count,
        in_specs=[VMEM] * 2,
        out_specs=[VMEM] * count,
        compiler_params=PARAMS,
        cost_estimate=pl.CostEstimate(flops=1_000_000, bytes_accessed=1_000_000, transcendentals=0),
    )(voltages, given)


def gather_half_kernel(steps, groups, select_ref, *rest):
    xs, outs = rest[: len(steps)], rest[len(steps) : len(steps) + groups]
    wide, pair = rest[len(steps) + groups :]
    inputs = xs[0].shape[0]
    each = inputs // 2
    chip = lax.axis_index("chan") // 2
    for i, (step, x) in enumerate(zip(steps, xs)):
        wide[i * inputs : (i + 1) * inputs] = x[...].astype(jnp.float32)
        pols = [wide[pl.ds(i * inputs + pol, each, stride=2), :] for pol in range(2)]
        top = (chip ^ step) * inputs
        for core, one in enumerate(fold(*pols)):
            pair[pl.ds(pl.multiple_of(top + core * each, each), each)] = one.astype(jnp.bfloat16)
    picked = jnp.dot(select_ref[...], pair[...], preferred_element_type=jnp.float32)
    per, rows, _ = outs[0].shape
    for g, out in enumerate(outs):
        for s in range(per):
            top = (g * per + s) * rows
            out[s] = picked[top : top + rows].astype(jnp.bfloat16)


def gather_half(select, xs, steps, groups, per):
    inputs, samples = xs[0].shape
    rows, antennas = select.shape
    return pl.pallas_call(
        functools.partial(gather_half_kernel, steps, groups),
        out_shape=[jax.ShapeDtypeStruct((per, rows // (groups * per), samples), jnp.bfloat16)] * groups,
        in_specs=[VMEM] * (1 + len(xs)),
        out_specs=[VMEM] * groups,
        scratch_shapes=[
            pltpu.VMEM((inputs * len(xs), samples), jnp.float32),
            pltpu.VMEM((antennas, samples), jnp.bfloat16),
        ],
        compiler_params=PARAMS,
        cost_estimate=pl.CostEstimate(
            flops=2 * rows * antennas * samples, bytes_accessed=4_000_000, transcendentals=0
        ),
    )(select, *xs)


def join_kernel(*refs):
    *parts, tall = refs
    count = len(parts) // 3
    for e in range(count):
        first, second, out = parts[e], parts[count + e], parts[2 * count + e]
        per, rows, _ = first.shape
        for s in range(per):
            for pol, one in enumerate(fold(first[s].astype(jnp.float32), second[s].astype(jnp.float32))):
                tall[e * per + s, pl.ds(pol, rows, stride=2), :] = one
            out[s] = tall[e * per + s].astype(jnp.bfloat16)


def join(first, second):
    per, rows, samples = first[0].shape
    count = len(first)
    return pl.pallas_call(
        join_kernel,
        out_shape=[jax.ShapeDtypeStruct((per, 2 * rows, samples), jnp.bfloat16)] * count,
        in_specs=[VMEM] * (2 * count),
        out_specs=[VMEM] * count,
        scratch_shapes=[pltpu.VMEM((count * per, 2 * rows, samples), jnp.float32)],
        compiler_params=PARAMS,
        cost_estimate=pl.CostEstimate(flops=1_000_000, bytes_accessed=2_000_000, transcendentals=0),
    )(*first, *second)


def load_pair(steps, xs, wide, pair):
    inputs = xs[0].shape[0]
    antennas = inputs // 2
    chip = lax.axis_index("chan") // 2
    for i, (step, x) in enumerate(zip(steps, xs)):
        wide[i * inputs : (i + 1) * inputs] = x[...].astype(jnp.float32)
        if len(steps) == 1:
            top = 0
        else:
            top = pl.multiple_of((chip ^ step) * antennas, antennas)
        for pol in range(2):
            pair[pl.ds(top, antennas), pol * LANES : (pol + 1) * LANES] = wide[
                pl.ds(i * inputs + pol, antennas, stride=2), :
            ].astype(jnp.bfloat16)


def store_rows(picked, tall, outs):
    rows = picked.shape[0]
    for pol in range(2):
        tall[pl.ds(pol, rows, stride=2), :] = picked[:, pol * LANES : (pol + 1) * LANES]
    slots = outs[0].shape[1]
    top = 0
    for out in outs:
        for s in range(out.shape[0]):
            out[s] = tall[top : top + slots, :].astype(jnp.bfloat16)
            top += slots


def gather_kernel(steps, outputs, select_ref, *rest):
    xs, outs = rest[: len(steps)], rest[len(steps) : len(steps) + outputs]
    wide, pair, tall = rest[len(steps) + outputs :]
    load_pair(steps, xs, wide, pair)
    picked = jnp.dot(select_ref[...], pair[...], preferred_element_type=jnp.float32)
    store_rows(picked, tall, outs)


def gather(select, xs, steps, groups, per, slots, apart=None):
    _, samples = xs[0].shape
    rows, antennas = select.shape
    heights = []
    for g in range(groups):
        heights += [1] * per if g == apart else [per]
    out = pl.pallas_call(
        functools.partial(gather_kernel, steps, len(heights)),
        out_shape=[jax.ShapeDtypeStruct((height, slots, samples), jnp.bfloat16) for height in heights],
        in_specs=[VMEM] * (1 + len(xs)),
        out_specs=[VMEM] * len(heights),
        scratch_shapes=[
            pltpu.VMEM((2 * antennas, samples), jnp.float32),
            pltpu.VMEM((antennas, 2 * samples), jnp.bfloat16),
            pltpu.VMEM((2 * rows, samples), jnp.float32),
        ],
        compiler_params=PARAMS,
        cost_estimate=pl.CostEstimate(
            flops=2 * rows * antennas * 2 * samples, bytes_accessed=4_000_000, transcendentals=0
        ),
    )(select, *xs)
    chunks = []
    for g in range(groups):
        chunks.append(list(out[:per]) if g == apart else out[0])
        out = out[per:] if g == apart else out[1:]
    return chunks


def products(real, imag):
    right = jnp.concatenate([real, imag], axis=1)
    left = jnp.concatenate([right, jnp.concatenate([imag, -real], axis=1)], axis=0)
    return lax.dot_general(left, right, (((1,), (1,)), ((), ())), preferred_element_type=jnp.float32)


def early_kernel(*refs):
    *parts, out = refs
    count = len(parts) // 2
    for s in range(parts[0].shape[0]):
        total = None
        for e in range(count):
            term = products(parts[e][s], parts[count + e][s])
            total = term if total is None else total + term
        out[s] = total


def late_kernel(slot, real, imag, so_far, *rest):
    out, stage, sem = rest[-3:]
    slots = real.shape[1]
    term = products(real[slot], imag[0])
    copies = []
    for part in range(2):
        stage[part] = so_far[slot, part * slots : (part + 1) * slots] + term[part * slots : (part + 1) * slots]
        copy = pltpu.make_async_copy(stage.at[part], out.at[slot, 0, part], sem.at[part])
        copy.start()
        copies.append(copy)
    for copy in copies:
        copy.wait()


def gram(real, imag, last):
    per, slots, samples = real[0].shape
    early = [e for e in range(len(real)) if e != last]
    flops = 2 * per * 2 * slots * slots * 2 * samples
    so_far = pl.pallas_call(
        early_kernel,
        out_shape=jax.ShapeDtypeStruct((per, 2 * slots, slots), jnp.float32),
        in_specs=[VMEM] * (2 * len(early)),
        out_specs=VMEM,
        compiler_params=PARAMS,
        cost_estimate=pl.CostEstimate(flops=flops * len(early), bytes_accessed=3_000_000, transcendentals=0),
    )(*[real[e] for e in early], *[imag[e] for e in early])
    anywhere = pl.BlockSpec(memory_space=pl.ANY)
    out = ()
    for s in range(per):
        out = pl.pallas_call(
            functools.partial(late_kernel, s),
            out_shape=[jax.ShapeDtypeStruct((per, 1, 2, slots, slots), jnp.float32)],
            in_specs=[VMEM] * 3 + [anywhere] * len(out),
            out_specs=[anywhere],
            scratch_shapes=[pltpu.VMEM((2, slots, slots), jnp.float32), pltpu.SemaphoreType.DMA((2,))],
            input_output_aliases={3: 0} if out else {},
            compiler_params=PARAMS,
            cost_estimate=pl.CostEstimate(flops=flops // per, bytes_accessed=2_000_000, transcendentals=0),
        )(real[last], imag[last][s], so_far, *out)
    return out[0]


def exchange(chunks, order, groups):
    got = list(chunks)
    for step in order:
        pairs = [(j, partner(j, step, groups)) for j in range(groups)]
        parts = chunks[step] if isinstance(chunks[step], list) else [chunks[step]]
        moved = []
        for part in parts:
            moved.append(lax.ppermute(part, "tm", pairs))
        got[step] = moved if len(parts) > 1 else moved[0]
    return got


def across(x):
    x = lax.all_to_all(x, "chan", split_axis=0, concat_axis=1, tiled=True)
    return x.reshape(x.shape[1], x.shape[2])


CHIP_ORDER = (3, 1, 2)


def cross(chunks, chans, starts):
    got = list(chunks)
    for step in CHIP_ORDER:
        if 2 * step < chans:
            got[step] = lax.ppermute(chunks[step], "chan", [(i, i ^ (2 * step)) for i in starts])
    return got


def by_chip(chans):
    return chans in (2, 4, 8)


def orders(groups):
    last = 2 if groups == 4 else groups - 1
    return [2,3,1], [3,1,2], last


def steps_of(voltages, assignment, slot_subarray_index):
    groups = lax.axis_size("tm")
    chans = lax.axis_size("chan")
    subarrays = slot_subarray_index.shape[0]
    per = subarrays // groups
    first, second, last = orders(groups)
    if not by_chip(chans):
        steps = (0,)
        reals = [across(voltages[0])]
        imags = [across(voltages[1])]
        select = plan(assignment, slot_subarray_index, groups, SLOT // 2)
        real = exchange(gather(select, reals, steps, groups, per, SLOT), first, groups)
        imag = exchange(gather(select, imags, steps, groups, per, SLOT, last), second, groups)
        return gram(real, imag, last)

    chips = chans // 2
    steps = tuple(range(chips))
    swap = [(i, i ^ 1) for i in range(chans)]
    given = lax.ppermute(give(voltages), "chan", swap)
    halves = merge(merge_halves_kernel, 1, voltages, given)
    select = plan(assignment, slot_subarray_index, groups, SLOT // 2)
    got = []
    for h in range(2):
        pieces = cross(halves[h * chips : (h + 1) * chips], chans, range(chans))
        got.append(exchange(gather_half(select, pieces, steps, groups, per), first, groups))
    imags = cross(merge(merge_kernel, 2, voltages, given), chans, range(chans))
    imag = exchange(gather(select, imags, steps, groups, per, SLOT, last), second, groups)
    return gram(join(*got), imag, last)


def solution(mesh):
    placed = (P(None, None, "chan", "tm"), P(), P())
    return jax.shard_map(
        steps_of,
        mesh=mesh,
        in_specs=placed,
        out_specs=P("tm", "chan", None, None, None),
        check_vma=False,
    )
```

```python
import functools

import jax
import jax.numpy as jnp
from jax import lax
from jax.experimental import pallas as pl
from jax.experimental.pallas import tpu as pltpu
from jax.sharding import PartitionSpec as P


SLOT = 384
LANES = 128


VMEM = pl.BlockSpec(memory_space=pltpu.VMEM)
PARAMS = pltpu.CompilerParams(vmem_limit_bytes=20 * 1024 * 1024)


def partner(index, step, count):
    if count & (count - 1):
        return lax.rem(index + step, count) if not isinstance(index, int) else (index + step) % count
    return index ^ step


def relative(owner, me, count):
    if count & (count - 1):
        return lax.rem(owner - me + count, count)
    return owner ^ me


def plan_kernel(groups, half, slot_ref, owner_ref, select_ref):
    subarrays = slot_ref.shape[1]
    blocks = owner_ref.shape[0]
    per = subarrays // groups
    me = lax.axis_index("tm")
    shape = (subarrays, LANES)
    place = lax.broadcasted_iota(jnp.int32, shape, 0)
    square = (subarrays, subarrays)
    diagonal = lax.broadcasted_iota(jnp.int32, square, 0) == lax.broadcasted_iota(jnp.int32, square, 1)
    slot = jnp.broadcast_to(slot_ref[...].astype(jnp.float32), square)
    name = jnp.sum(jnp.where(diagonal, slot, 0.0), axis=1, keepdims=True)
    name = jnp.broadcast_to(name, shape).astype(jnp.int32)
    base = jnp.zeros(shape, jnp.int32)
    for s in range(subarrays):
        chunk = relative(jnp.int32(s // per), me, groups) * per + s % per
        base = jnp.where(place == s, chunk * half, base)
    base = base.astype(jnp.float32)
    earlier = lax.broadcasted_iota(jnp.int32, (LANES, LANES), 0)
    later = lax.broadcasted_iota(jnp.int32, (LANES, LANES), 1)
    before = jnp.where(earlier < later, 1.0, 0.0).astype(jnp.bfloat16)
    held = [jnp.where(owner_ref[b : b + 1, :] == name, 1.0, 0.0) for b in range(blocks)]
    within = jnp.dot(
        jnp.concatenate(held, axis=0).astype(jnp.bfloat16), before, preferred_element_type=jnp.float32
    )
    run = base
    height, strip = 256, 16
    rows = lax.broadcasted_iota(jnp.int32, (strip, LANES), 0)
    strips = [(rows + top).astype(jnp.float32).astype(jnp.bfloat16) for top in range(0, height, strip)]
    one, zero = jnp.ones((strip, LANES), jnp.bfloat16), jnp.zeros((strip, LANES), jnp.bfloat16)
    for b in range(blocks):
        rank = within[b * subarrays : (b + 1) * subarrays] + run
        target = jnp.sum(held[b] * rank, axis=0, keepdims=True)
        run = run + jnp.sum(held[b], axis=1, keepdims=True)
        for top in range(0, select_ref.shape[0], height):
            inside = jnp.logical_and(target >= top, target < top + height)
            at = jnp.where(inside, target - top, -1.0)
            at = jnp.broadcast_to(at, (strip, LANES)).astype(jnp.bfloat16)
            for i, row in enumerate(strips):
                start = top + i * strip
                select_ref[start : start + strip, b * LANES : (b + 1) * LANES] = jnp.where(row == at, one, zero)


def plan(assignment, slot_subarray_index, groups, half):
    antennas = assignment.shape[0]
    subarrays = slot_subarray_index.shape[0]
    return pl.pallas_call(
        functools.partial(plan_kernel, groups, half),
        out_shape=jax.ShapeDtypeStruct((subarrays * half, antennas), jnp.bfloat16),
        in_specs=[VMEM, VMEM],
        out_specs=VMEM,
        compiler_params=PARAMS,
        cost_estimate=pl.CostEstimate(flops=4_000_000_000, bytes_accessed=3_000_000, transcendentals=0),
    )(slot_subarray_index.reshape(1, subarrays), assignment.reshape(antennas // LANES, LANES))


def give_kernel(chips, x_ref, out):
    me = lax.axis_index("chan")
    for k in range(2):
        for t in range(chips):
            out[k, t] = x_ref[k, (me ^ (2 * t)) ^ 1]


def give(voltages):
    parts, chans, inputs, samples = voltages.shape
    return pl.pallas_call(
        functools.partial(give_kernel, chans // 2),
        out_shape=jax.ShapeDtypeStruct((parts, chans // 2, inputs, samples), voltages.dtype),
        in_specs=[VMEM],
        out_specs=VMEM,
        compiler_params=PARAMS,
        cost_estimate=pl.CostEstimate(flops=1_000_000, bytes_accessed=1_000_000, transcendentals=0),
    )(voltages)


def fold(a, b):
    half = LANES // 2
    left = lax.broadcasted_iota(jnp.int32, a.shape, 1) < half
    return (
        jnp.where(left, a, pltpu.roll(b, half, 1)),
        jnp.where(left, pltpu.roll(a, half, 1), b),
    )


def merge_halves_kernel(chips, x_ref, given_ref, *outs):
    me = lax.axis_index("chan")
    for parity in range(2):

        @pl.when((me & 1) == parity)
        def _():
            for t in range(chips):
                cores = [x_ref[0, me ^ (2 * t)], given_ref[0, t]]
                if parity:
                    cores.reverse()
                for h, half in enumerate(fold(*[core.astype(jnp.float32) for core in cores])):
                    outs[h * chips + t][...] = half.astype(jnp.bfloat16)


def merge_kernel(chips, x_ref, given_ref, *outs):
    me = lax.axis_index("chan")
    inputs = x_ref.shape[2]
    mine = pl.multiple_of((me & 1) * inputs, inputs)
    theirs = pl.multiple_of(inputs - (me & 1) * inputs, inputs)
    for t in range(chips):
        outs[t][pl.ds(mine, inputs)] = x_ref[1, me ^ (2 * t)]
        outs[t][pl.ds(theirs, inputs)] = given_ref[1, t]


def merge(kernel, height, voltages, given):
    _, chans, inputs, samples = voltages.shape
    chips = chans // 2
    count = 2 * chips // height
    return pl.pallas_call(
        functools.partial(kernel, chips),
        out_shape=[jax.ShapeDtypeStruct((height * inputs, samples), voltages.dtype)] * count,
        in_specs=[VMEM] * 2,
        out_specs=[VMEM] * count,
        compiler_params=PARAMS,
        cost_estimate=pl.CostEstimate(flops=1_000_000, bytes_accessed=1_000_000, transcendentals=0),
    )(voltages, given)


def gather_half_kernel(steps, groups, select_ref, *rest):
    xs, outs = rest[: len(steps)], rest[len(steps) : len(steps) + groups]
    wide, pair = rest[len(steps) + groups :]
    inputs = xs[0].shape[0]
    each = inputs // 2
    chip = lax.axis_index("chan") // 2
    for i, (step, x) in enumerate(zip(steps, xs)):
        wide[i * inputs : (i + 1) * inputs] = x[...].astype(jnp.float32)
        pols = [wide[pl.ds(i * inputs + pol, each, stride=2), :] for pol in range(2)]
        top = (chip ^ step) * inputs
        for core, one in enumerate(fold(*pols)):
            pair[pl.ds(pl.multiple_of(top + core * each, each), each)] = one.astype(jnp.bfloat16)
    picked = jnp.dot(select_ref[...], pair[...], preferred_element_type=jnp.float32)
    per, rows, _ = outs[0].shape
    for g, out in enumerate(outs):
        for s in range(per):
            top = (g * per + s) * rows
            out[s] = picked[top : top + rows].astype(jnp.bfloat16)


def gather_half(select, xs, steps, groups, per):
    inputs, samples = xs[0].shape
    rows, antennas = select.shape
    return pl.pallas_call(
        functools.partial(gather_half_kernel, steps, groups),
        out_shape=[jax.ShapeDtypeStruct((per, rows // (groups * per), samples), jnp.bfloat16)] * groups,
        in_specs=[VMEM] * (1 + len(xs)),
        out_specs=[VMEM] * groups,
        scratch_shapes=[
            pltpu.VMEM((inputs * len(xs), samples), jnp.float32),
            pltpu.VMEM((antennas, samples), jnp.bfloat16),
        ],
        compiler_params=PARAMS,
        cost_estimate=pl.CostEstimate(
            flops=2 * rows * antennas * samples, bytes_accessed=4_000_000, transcendentals=0
        ),
    )(select, *xs)


def join_kernel(*refs):
    *parts, tall = refs
    count = len(parts) // 3
    for e in range(count):
        first, second, out = parts[e], parts[count + e], parts[2 * count + e]
        per, rows, _ = first.shape
        for s in range(per):
            for pol, one in enumerate(fold(first[s].astype(jnp.float32), second[s].astype(jnp.float32))):
                tall[e * per + s, pl.ds(pol, rows, stride=2), :] = one
            out[s] = tall[e * per + s].astype(jnp.bfloat16)


def join(first, second):
    per, rows, samples = first[0].shape
    count = len(first)
    return pl.pallas_call(
        join_kernel,
        out_shape=[jax.ShapeDtypeStruct((per, 2 * rows, samples), jnp.bfloat16)] * count,
        in_specs=[VMEM] * (2 * count),
        out_specs=[VMEM] * count,
        scratch_shapes=[pltpu.VMEM((count * per, 2 * rows, samples), jnp.float32)],
        compiler_params=PARAMS,
        cost_estimate=pl.CostEstimate(flops=1_000_000, bytes_accessed=2_000_000, transcendentals=0),
    )(*first, *second)


def load_pair(steps, xs, wide, pair):
    inputs = xs[0].shape[0]
    antennas = inputs // 2
    chip = lax.axis_index("chan") // 2
    for i, (step, x) in enumerate(zip(steps, xs)):
        wide[i * inputs : (i + 1) * inputs] = x[...].astype(jnp.float32)
        if len(steps) == 1:
            top = 0
        else:
            top = pl.multiple_of((chip ^ step) * antennas, antennas)
        for pol in range(2):
            pair[pl.ds(top, antennas), pol * LANES : (pol + 1) * LANES] = wide[
                pl.ds(i * inputs + pol, antennas, stride=2), :
            ].astype(jnp.bfloat16)


def store_rows(picked, tall, outs):
    rows = picked.shape[0]
    for pol in range(2):
        tall[pl.ds(pol, rows, stride=2), :] = picked[:, pol * LANES : (pol + 1) * LANES]
    slots = outs[0].shape[1]
    top = 0
    for out in outs:
        for s in range(out.shape[0]):
            out[s] = tall[top : top + slots, :].astype(jnp.bfloat16)
            top += slots


def gather_kernel(steps, outputs, select_ref, *rest):
    xs, outs = rest[: len(steps)], rest[len(steps) : len(steps) + outputs]
    wide, pair, tall = rest[len(steps) + outputs :]
    load_pair(steps, xs, wide, pair)
    picked = jnp.dot(select_ref[...], pair[...], preferred_element_type=jnp.float32)
    store_rows(picked, tall, outs)


def gather(select, xs, steps, groups, per, slots, apart=None):
    _, samples = xs[0].shape
    rows, antennas = select.shape
    heights = []
    for g in range(groups):
        heights += [1] * per if g == apart else [per]
    out = pl.pallas_call(
        functools.partial(gather_kernel, steps, len(heights)),
        out_shape=[jax.ShapeDtypeStruct((height, slots, samples), jnp.bfloat16) for height in heights],
        in_specs=[VMEM] * (1 + len(xs)),
        out_specs=[VMEM] * len(heights),
        scratch_shapes=[
            pltpu.VMEM((2 * antennas, samples), jnp.float32),
            pltpu.VMEM((antennas, 2 * samples), jnp.bfloat16),
            pltpu.VMEM((2 * rows, samples), jnp.float32),
        ],
        compiler_params=PARAMS,
        cost_estimate=pl.CostEstimate(
            flops=2 * rows * antennas * 2 * samples, bytes_accessed=4_000_000, transcendentals=0
        ),
    )(select, *xs)
    chunks = []
    for g in range(groups):
        chunks.append(list(out[:per]) if g == apart else out[0])
        out = out[per:] if g == apart else out[1:]
    return chunks


def products(real, imag):
    right = jnp.concatenate([real, imag], axis=1)
    left = jnp.concatenate([right, jnp.concatenate([imag, -real], axis=1)], axis=0)
    return lax.dot_general(left, right, (((1,), (1,)), ((), ())), preferred_element_type=jnp.float32)


def early_kernel(*refs):
    *parts, out = refs
    count = len(parts) // 2
    for s in range(parts[0].shape[0]):
        total = None
        for e in range(count):
            term = products(parts[e][s], parts[count + e][s])
            total = term if total is None else total + term
        out[s] = total


def late_kernel(slot, real, imag, so_far, *rest):
    out, stage, sem = rest[-3:]
    slots = real.shape[1]
    term = products(real[slot], imag[0])
    copies = []
    for part in range(2):
        stage[part] = so_far[slot, part * slots : (part + 1) * slots] + term[part * slots : (part + 1) * slots]
        copy = pltpu.make_async_copy(stage.at[part], out.at[slot, 0, part], sem.at[part])
        copy.start()
        copies.append(copy)
    for copy in copies:
        copy.wait()


def gram(real, imag, last):
    per, slots, samples = real[0].shape
    early = [e for e in range(len(real)) if e != last]
    flops = 2 * per * 2 * slots * slots * 2 * samples
    so_far = pl.pallas_call(
        early_kernel,
        out_shape=jax.ShapeDtypeStruct((per, 2 * slots, slots), jnp.float32),
        in_specs=[VMEM] * (2 * len(early)),
        out_specs=VMEM,
        compiler_params=PARAMS,
        cost_estimate=pl.CostEstimate(flops=flops * len(early), bytes_accessed=3_000_000, transcendentals=0),
    )(*[real[e] for e in early], *[imag[e] for e in early])
    anywhere = pl.BlockSpec(memory_space=pl.ANY)
    out = ()
    for s in range(per):
        out = pl.pallas_call(
            functools.partial(late_kernel, s),
            out_shape=[jax.ShapeDtypeStruct((per, 1, 2, slots, slots), jnp.float32)],
            in_specs=[VMEM] * 3 + [anywhere] * len(out),
            out_specs=[anywhere],
            scratch_shapes=[pltpu.VMEM((2, slots, slots), jnp.float32), pltpu.SemaphoreType.DMA((2,))],
            input_output_aliases={3: 0} if out else {},
            compiler_params=PARAMS,
            cost_estimate=pl.CostEstimate(flops=flops // per, bytes_accessed=2_000_000, transcendentals=0),
        )(real[last], imag[last][s], so_far, *out)
    return out[0]


def exchange(chunks, order, groups):
    got = list(chunks)
    for step in order:
        pairs = [(j, partner(j, step, groups)) for j in range(groups)]
        parts = chunks[step] if isinstance(chunks[step], list) else [chunks[step]]
        moved = []
        for part in parts:
            moved.append(lax.ppermute(part, "tm", pairs))
        got[step] = moved if len(parts) > 1 else moved[0]
    return got


def across(x):
    x = lax.all_to_all(x, "chan", split_axis=0, concat_axis=1, tiled=True)
    return x.reshape(x.shape[1], x.shape[2])


CHIP_ORDER = (3, 1, 2)


def cross(chunks, chans, starts):
    got = list(chunks)
    for step in CHIP_ORDER:
        if 2 * step < chans:
            got[step] = lax.ppermute(chunks[step], "chan", [(i, i ^ (2 * step)) for i in starts])
    return got


def by_chip(chans):
    return chans in (2, 4, 8)


def orders(groups):
    if groups == 4:
        return [2, 3, 1], [2, 1, 3], 3
    rest = list(range(groups - 2, 0, -1))
    return [groups - 1] + rest, rest + [groups - 1], groups - 1


def steps_of(voltages, assignment, slot_subarray_index):
    groups = lax.axis_size("tm")
    chans = lax.axis_size("chan")
    subarrays = slot_subarray_index.shape[0]
    per = subarrays // groups
    first, second, last = orders(groups)
    if not by_chip(chans):
        steps = (0,)
        reals = [across(voltages[0])]
        imags = [across(voltages[1])]
        select = plan(assignment, slot_subarray_index, groups, SLOT // 2)
        real = exchange(gather(select, reals, steps, groups, per, SLOT), first, groups)
        imag = exchange(gather(select, imags, steps, groups, per, SLOT, last), second, groups)
        return gram(real, imag, last)

    chips = chans // 2
    steps = tuple(range(chips))
    swap = [(i, i ^ 1) for i in range(chans)]
    given = lax.ppermute(give(voltages), "chan", swap)
    halves = merge(merge_halves_kernel, 1, voltages, given)
    select = plan(assignment, slot_subarray_index, groups, SLOT // 2)
    got = []
    for h in range(2):
        pieces = cross(halves[h * chips : (h + 1) * chips], chans, range(chans))
        got.append(exchange(gather_half(select, pieces, steps, groups, per), first, groups))
    imags = cross(merge(merge_kernel, 2, voltages, given), chans, range(chans))
    imag = exchange(gather(select, imags, steps, groups, per, SLOT, last), second, groups)
    return gram(join(*got), imag, last)


def solution(mesh):
    placed = (P(None, None, "chan", "tm"), P(), P())
    return jax.shard_map(
        steps_of,
        mesh=mesh,
        in_specs=placed,
        out_specs=P("tm", "chan", None, None, None),
        check_vma=False,
    )
```

```python
import functools

import jax
import jax.numpy as jnp
from jax import lax
from jax.experimental import pallas as pl
from jax.experimental.pallas import tpu as pltpu
from jax.sharding import PartitionSpec as P


SLOT = 384
LANES = 128


VMEM = pl.BlockSpec(memory_space=pltpu.VMEM)
PARAMS = pltpu.CompilerParams(vmem_limit_bytes=20 * 1024 * 1024)


def partner(index, step, count):
    if count & (count - 1):
        return lax.rem(index + step, count) if not isinstance(index, int) else (index + step) % count
    return index ^ step


def relative(owner, me, count):
    if count & (count - 1):
        return lax.rem(owner - me + count, count)
    return owner ^ me


def plan_kernel(groups, half, slot_ref, owner_ref, select_ref):
    subarrays = slot_ref.shape[1]
    blocks = owner_ref.shape[0]
    per = subarrays // groups
    me = lax.axis_index("tm")
    shape = (subarrays, LANES)
    place = lax.broadcasted_iota(jnp.int32, shape, 0)
    square = (subarrays, subarrays)
    diagonal = lax.broadcasted_iota(jnp.int32, square, 0) == lax.broadcasted_iota(jnp.int32, square, 1)
    slot = jnp.broadcast_to(slot_ref[...].astype(jnp.float32), square)
    name = jnp.sum(jnp.where(diagonal, slot, 0.0), axis=1, keepdims=True)
    name = jnp.broadcast_to(name, shape).astype(jnp.int32)
    base = jnp.zeros(shape, jnp.int32)
    for s in range(subarrays):
        chunk = relative(jnp.int32(s // per), me, groups) * per + s % per
        base = jnp.where(place == s, chunk * half, base)
    base = base.astype(jnp.float32)
    earlier = lax.broadcasted_iota(jnp.int32, (LANES, LANES), 0)
    later = lax.broadcasted_iota(jnp.int32, (LANES, LANES), 1)
    before = jnp.where(earlier < later, 1.0, 0.0).astype(jnp.bfloat16)
    held = [jnp.where(owner_ref[b : b + 1, :] == name, 1.0, 0.0) for b in range(blocks)]
    within = jnp.dot(
        jnp.concatenate(held, axis=0).astype(jnp.bfloat16), before, preferred_element_type=jnp.float32
    )
    run = base
    height, strip = 256, 16
    rows = lax.broadcasted_iota(jnp.int32, (strip, LANES), 0)
    strips = [(rows + top).astype(jnp.float32).astype(jnp.bfloat16) for top in range(0, height, strip)]
    one, zero = jnp.ones((strip, LANES), jnp.bfloat16), jnp.zeros((strip, LANES), jnp.bfloat16)
    for b in range(blocks):
        rank = within[b * subarrays : (b + 1) * subarrays] + run
        target = jnp.sum(held[b] * rank, axis=0, keepdims=True)
        run = run + jnp.sum(held[b], axis=1, keepdims=True)
        for top in range(0, select_ref.shape[0], height):
            inside = jnp.logical_and(target >= top, target < top + height)
            at = jnp.where(inside, target - top, -1.0)
            at = jnp.broadcast_to(at, (strip, LANES)).astype(jnp.bfloat16)
            for i, row in enumerate(strips):
                start = top + i * strip
                select_ref[start : start + strip, b * LANES : (b + 1) * LANES] = jnp.where(row == at, one, zero)


def plan(assignment, slot_subarray_index, groups, half):
    antennas = assignment.shape[0]
    subarrays = slot_subarray_index.shape[0]
    return pl.pallas_call(
        functools.partial(plan_kernel, groups, half),
        out_shape=jax.ShapeDtypeStruct((subarrays * half, antennas), jnp.bfloat16),
        in_specs=[VMEM, VMEM],
        out_specs=VMEM,
        compiler_params=PARAMS,
        cost_estimate=pl.CostEstimate(flops=4_000_000_000, bytes_accessed=3_000_000, transcendentals=0),
    )(slot_subarray_index.reshape(1, subarrays), assignment.reshape(antennas // LANES, LANES))


def give_kernel(chips, x_ref, out):
    me = lax.axis_index("chan")
    for k in range(2):
        for t in range(chips):
            out[k, t] = x_ref[k, (me ^ (2 * t)) ^ 1]


def give(voltages):
    parts, chans, inputs, samples = voltages.shape
    return pl.pallas_call(
        functools.partial(give_kernel, chans // 2),
        out_shape=jax.ShapeDtypeStruct((parts, chans // 2, inputs, samples), voltages.dtype),
        in_specs=[VMEM],
        out_specs=VMEM,
        compiler_params=PARAMS,
        cost_estimate=pl.CostEstimate(flops=1_000_000, bytes_accessed=1_000_000, transcendentals=0),
    )(voltages)


def fold(a, b):
    half = LANES // 2
    left = lax.broadcasted_iota(jnp.int32, a.shape, 1) < half
    return (
        jnp.where(left, a, pltpu.roll(b, half, 1)),
        jnp.where(left, pltpu.roll(a, half, 1), b),
    )


def merge_halves_kernel(chips, x_ref, given_ref, *outs):
    me = lax.axis_index("chan")
    for parity in range(2):

        @pl.when((me & 1) == parity)
        def _():
            for t in range(chips):
                cores = [x_ref[0, me ^ (2 * t)], given_ref[0, t]]
                if parity:
                    cores.reverse()
                for h, half in enumerate(fold(*[core.astype(jnp.float32) for core in cores])):
                    outs[h * chips + t][...] = half.astype(jnp.bfloat16)


def merge_kernel(chips, x_ref, given_ref, *outs):
    me = lax.axis_index("chan")
    inputs = x_ref.shape[2]
    mine = pl.multiple_of((me & 1) * inputs, inputs)
    theirs = pl.multiple_of(inputs - (me & 1) * inputs, inputs)
    for t in range(chips):
        outs[t][pl.ds(mine, inputs)] = x_ref[1, me ^ (2 * t)]
        outs[t][pl.ds(theirs, inputs)] = given_ref[1, t]


def merge(kernel, height, voltages, given):
    _, chans, inputs, samples = voltages.shape
    chips = chans // 2
    count = 2 * chips // height
    return pl.pallas_call(
        functools.partial(kernel, chips),
        out_shape=[jax.ShapeDtypeStruct((height * inputs, samples), voltages.dtype)] * count,
        in_specs=[VMEM] * 2,
        out_specs=[VMEM] * count,
        compiler_params=PARAMS,
        cost_estimate=pl.CostEstimate(flops=1_000_000, bytes_accessed=1_000_000, transcendentals=0),
    )(voltages, given)


def gather_half_kernel(steps, groups, select_ref, *rest):
    xs, outs = rest[: len(steps)], rest[len(steps) : len(steps) + groups]
    wide, pair = rest[len(steps) + groups :]
    inputs = xs[0].shape[0]
    each = inputs // 2
    chip = lax.axis_index("chan") // 2
    for i, (step, x) in enumerate(zip(steps, xs)):
        wide[i * inputs : (i + 1) * inputs] = x[...].astype(jnp.float32)
        pols = [wide[pl.ds(i * inputs + pol, each, stride=2), :] for pol in range(2)]
        top = (chip ^ step) * inputs
        for core, one in enumerate(fold(*pols)):
            pair[pl.ds(pl.multiple_of(top + core * each, each), each)] = one.astype(jnp.bfloat16)
    picked = jnp.dot(select_ref[...], pair[...], preferred_element_type=jnp.float32)
    per, rows, _ = outs[0].shape
    for g, out in enumerate(outs):
        for s in range(per):
            top = (g * per + s) * rows
            out[s] = picked[top : top + rows].astype(jnp.bfloat16)


def gather_half(select, xs, steps, groups, per):
    inputs, samples = xs[0].shape
    rows, antennas = select.shape
    return pl.pallas_call(
        functools.partial(gather_half_kernel, steps, groups),
        out_shape=[jax.ShapeDtypeStruct((per, rows // (groups * per), samples), jnp.bfloat16)] * groups,
        in_specs=[VMEM] * (1 + len(xs)),
        out_specs=[VMEM] * groups,
        scratch_shapes=[
            pltpu.VMEM((inputs * len(xs), samples), jnp.float32),
            pltpu.VMEM((antennas, samples), jnp.bfloat16),
        ],
        compiler_params=PARAMS,
        cost_estimate=pl.CostEstimate(
            flops=2 * rows * antennas * samples, bytes_accessed=4_000_000, transcendentals=0
        ),
    )(select, *xs)


def join_kernel(*refs):
    *parts, tall = refs
    count = len(parts) // 3
    for e in range(count):
        first, second, out = parts[e], parts[count + e], parts[2 * count + e]
        per, rows, _ = first.shape
        for s in range(per):
            for pol, one in enumerate(fold(first[s].astype(jnp.float32), second[s].astype(jnp.float32))):
                tall[e * per + s, pl.ds(pol, rows, stride=2), :] = one
            out[s] = tall[e * per + s].astype(jnp.bfloat16)


def join(first, second):
    per, rows, samples = first[0].shape
    count = len(first)
    return pl.pallas_call(
        join_kernel,
        out_shape=[jax.ShapeDtypeStruct((per, 2 * rows, samples), jnp.bfloat16)] * count,
        in_specs=[VMEM] * (2 * count),
        out_specs=[VMEM] * count,
        scratch_shapes=[pltpu.VMEM((count * per, 2 * rows, samples), jnp.float32)],
        compiler_params=PARAMS,
        cost_estimate=pl.CostEstimate(flops=1_000_000, bytes_accessed=2_000_000, transcendentals=0),
    )(*first, *second)


def load_pair(steps, xs, wide, pair):
    inputs = xs[0].shape[0]
    antennas = inputs // 2
    chip = lax.axis_index("chan") // 2
    for i, (step, x) in enumerate(zip(steps, xs)):
        wide[i * inputs : (i + 1) * inputs] = x[...].astype(jnp.float32)
        if len(steps) == 1:
            top = 0
        else:
            top = pl.multiple_of((chip ^ step) * antennas, antennas)
        for pol in range(2):
            pair[pl.ds(top, antennas), pol * LANES : (pol + 1) * LANES] = wide[
                pl.ds(i * inputs + pol, antennas, stride=2), :
            ].astype(jnp.bfloat16)


def store_rows(picked, tall, outs):
    rows = picked.shape[0]
    for pol in range(2):
        tall[pl.ds(pol, rows, stride=2), :] = picked[:, pol * LANES : (pol + 1) * LANES]
    slots = outs[0].shape[1]
    top = 0
    for out in outs:
        for s in range(out.shape[0]):
            out[s] = tall[top : top + slots, :].astype(jnp.bfloat16)
            top += slots


def gather_kernel(steps, outputs, select_ref, *rest):
    xs, outs = rest[: len(steps)], rest[len(steps) : len(steps) + outputs]
    wide, pair, tall = rest[len(steps) + outputs :]
    load_pair(steps, xs, wide, pair)
    picked = jnp.dot(select_ref[...], pair[...], preferred_element_type=jnp.float32)
    store_rows(picked, tall, outs)


def gather(select, xs, steps, groups, per, slots, apart=None):
    _, samples = xs[0].shape
    rows, antennas = select.shape
    heights = []
    for g in range(groups):
        heights += [1] * per if g == apart else [per]
    out = pl.pallas_call(
        functools.partial(gather_kernel, steps, len(heights)),
        out_shape=[jax.ShapeDtypeStruct((height, slots, samples), jnp.bfloat16) for height in heights],
        in_specs=[VMEM] * (1 + len(xs)),
        out_specs=[VMEM] * len(heights),
        scratch_shapes=[
            pltpu.VMEM((2 * antennas, samples), jnp.float32),
            pltpu.VMEM((antennas, 2 * samples), jnp.bfloat16),
            pltpu.VMEM((2 * rows, samples), jnp.float32),
        ],
        compiler_params=PARAMS,
        cost_estimate=pl.CostEstimate(
            flops=2 * rows * antennas * 2 * samples, bytes_accessed=4_000_000, transcendentals=0
        ),
    )(select, *xs)
    chunks = []
    for g in range(groups):
        chunks.append(list(out[:per]) if g == apart else out[0])
        out = out[per:] if g == apart else out[1:]
    return chunks


def products(real, imag):
    right = jnp.concatenate([real, imag], axis=1)
    left = jnp.concatenate([right, jnp.concatenate([imag, -real], axis=1)], axis=0)
    return lax.dot_general(left, right, (((1,), (1,)), ((), ())), preferred_element_type=jnp.float32)


def early_kernel(*refs):
    *parts, out = refs
    count = len(parts) // 2
    for s in range(parts[0].shape[0]):
        total = None
        for e in range(count):
            term = products(parts[e][s], parts[count + e][s])
            total = term if total is None else total + term
        out[s] = total


def late_kernel(real, *rest):
    *imags, so_far, out, stage, sem = rest
    slots = real.shape[1]
    copies = []
    for s, imag in enumerate(imags):
        term = products(real[s], imag[0])
        for part in range(2):
            rows = slice(part * slots, (part + 1) * slots)
            stage[s, part] = so_far[s, rows] + term[rows]
            copy = pltpu.make_async_copy(stage.at[s, part], out.at[s, 0, part], sem.at[s, part])
            copy.start()
            copies.append(copy)
    for copy in copies:
        copy.wait()


def gram(real, imag, last):
    per, slots, samples = real[0].shape
    early = [e for e in range(len(real)) if e != last]
    flops = 2 * per * 2 * slots * slots * 2 * samples
    so_far = pl.pallas_call(
        early_kernel,
        out_shape=jax.ShapeDtypeStruct((per, 2 * slots, slots), jnp.float32),
        in_specs=[VMEM] * (2 * len(early)),
        out_specs=VMEM,
        compiler_params=PARAMS,
        cost_estimate=pl.CostEstimate(flops=flops * len(early), bytes_accessed=3_000_000, transcendentals=0),
    )(*[real[e] for e in early], *[imag[e] for e in early])
    return pl.pallas_call(
        late_kernel,
        out_shape=jax.ShapeDtypeStruct((per, 1, 2, slots, slots), jnp.float32),
        in_specs=[VMEM] * (2 + per),
        out_specs=pl.BlockSpec(memory_space=pl.ANY),
        scratch_shapes=[pltpu.VMEM((per, 2, slots, slots), jnp.float32), pltpu.SemaphoreType.DMA((per, 2))],
        compiler_params=PARAMS,
        cost_estimate=pl.CostEstimate(flops=flops, bytes_accessed=3_000_000, transcendentals=0),
    )(real[last], *imag[last], so_far)


def exchange(chunks, order, groups):
    got = list(chunks)
    for step in order:
        pairs = [(j, partner(j, step, groups)) for j in range(groups)]
        parts = chunks[step] if isinstance(chunks[step], list) else [chunks[step]]
        moved = []
        for part in parts:
            moved.append(lax.ppermute(part, "tm", pairs))
        got[step] = moved if len(parts) > 1 else moved[0]
    return got


def across(x):
    x = lax.all_to_all(x, "chan", split_axis=0, concat_axis=1, tiled=True)
    return x.reshape(x.shape[1], x.shape[2])


CHIP_ORDER = (3, 1, 2)


def cross(chunks, chans, starts):
    got = list(chunks)
    for step in CHIP_ORDER:
        if 2 * step < chans:
            got[step] = lax.ppermute(chunks[step], "chan", [(i, i ^ (2 * step)) for i in starts])
    return got


def by_chip(chans):
    return chans in (2, 4, 8)


def orders(groups):
    if groups == 4:
        return [2, 3, 1], [2, 1, 3], 3
    rest = list(range(groups - 2, 0, -1))
    return [groups - 1] + rest, rest + [groups - 1], groups - 1


def steps_of(voltages, assignment, slot_subarray_index):
    groups = lax.axis_size("tm")
    chans = lax.axis_size("chan")
    subarrays = slot_subarray_index.shape[0]
    per = subarrays // groups
    first, second, last = orders(groups)
    if not by_chip(chans):
        steps = (0,)
        reals = [across(voltages[0])]
        imags = [across(voltages[1])]
        select = plan(assignment, slot_subarray_index, groups, SLOT // 2)
        real = exchange(gather(select, reals, steps, groups, per, SLOT), first, groups)
        imag = exchange(gather(select, imags, steps, groups, per, SLOT, last), second, groups)
        return gram(real, imag, last)

    chips = chans // 2
    steps = tuple(range(chips))
    swap = [(i, i ^ 1) for i in range(chans)]
    given = lax.ppermute(give(voltages), "chan", swap)
    halves = merge(merge_halves_kernel, 1, voltages, given)
    select = plan(assignment, slot_subarray_index, groups, SLOT // 2)
    got = []
    for h in range(2):
        pieces = cross(halves[h * chips : (h + 1) * chips], chans, range(chans))
        got.append(exchange(gather_half(select, pieces, steps, groups, per), first, groups))
    imags = cross(merge(merge_kernel, 2, voltages, given), chans, range(chans))
    imag = exchange(gather(select, imags, steps, groups, per, SLOT, last), second, groups)
    return gram(join(*got), imag, last)


def solution(mesh):
    placed = (P(None, None, "chan", "tm"), P(), P())
    return jax.shard_map(
        steps_of,
        mesh=mesh,
        in_specs=placed,
        out_specs=P("tm", "chan", None, None, None),
        check_vma=False,
    )
```
